256 devices in a mesh: freq: 8 (over x, core), rec: 32 (over z, y).
Axes of the slice: x: 4, y: 4, z: 8, core: 2. Of those that a mesh axis runs over, the one named last changes fastest.
Arguments:
- response_real: float32 [96, 1536, 1536], P('freq', 'rec'), may hold values from -0.109375 to 0.109375
- response_imaginary: float32 [96, 1536, 1536], P('freq', 'rec'), may hold values from -0.109375 to 0.109375
- focus: float32 [1536, 96, 128], P('rec', 'freq'), may hold values from -6 to 6
- initial: float32 [1536, 96, 128], P('rec', 'freq'), may hold values from -6 to 6
- onset: int32 [1536, 64], P('rec'), may hold values from 24 to 167
Outputs:
- focus_next: float32 [1536, 96, 128], P('rec', 'freq')
The draws below stay inside these ranges and needn't reach their ends.
All inputs are finite; a program needn't handle non-finite values.
Results may differ from the reference program's by a relative error of at most 0.0003.
Values sent between devices are 32-bit elements; how exact they have to be, the bound alone decides.
A program may use at most 128 MiB of HBM per device.

```python
import math
import jax
import jax.numpy as jnp
from jax import lax

F = 96
NPOS = 1536
P_SIZE = 64
NT = 192


def set_ends(drawn, own_key, least, top_value):
    dims = drawn.shape
    place = [jax.random.randint(jax.random.fold_in(own_key, axis), (), 0, dims[axis]) for axis in range(len(dims))]
    drawn = drawn.at[tuple(place)].set(least)
    longest = dims.index(max(dims))
    place[longest] = (place[longest] + 1) % dims[longest]
    return drawn.at[tuple(place)].set(top_value)


def shard_levels(stream_key, shape, pieces, smallest, top_value):
    factor_of = 1.0
    for axis_at, blocks in pieces:
        steps = jax.random.uniform(jax.random.fold_in(jax.random.fold_in(stream_key, 6), axis_at), (blocks,), jnp.float32, smallest / len(pieces), top_value / len(pieces))
        factor_of = factor_of * jnp.repeat(jnp.exp(steps), shape[axis_at] // blocks).reshape((-1,) + (1,) * (len(shape) - 1 - axis_at))
    return factor_of


def scatter_about(stream_key, dims, spread, most, cuts=(), held_as=jnp.bfloat16):
    level = shard_levels(stream_key, dims, cuts, -0.22, 0.18) if cuts else 1.0
    values = jax.random.normal(stream_key, dims, jnp.float32) * spread * level
    return jnp.minimum(jnp.maximum(values, -most), most).astype(held_as)


def setup_inputs(seed: int = 0) -> dict:
    key_of = jax.random.split(jax.random.key(seed), 6)
    return {
        "response_real": scatter_about(key_of[0], (F, NPOS, NPOS), (2 * NPOS) ** -0.5, 0.109375, ((0, 8), (1, 32)), jnp.float32),
        "response_imaginary": scatter_about(key_of[1], (F, NPOS, NPOS), (2 * NPOS) ** -0.5, 0.109375, ((0, 8), (1, 32)), jnp.float32),
        "focus": scatter_about(key_of[2], (NPOS, F, 2 * P_SIZE), 1.0, 6.0, ((0, 32), (1, 8)), jnp.float32),
        "initial": scatter_about(key_of[3], (NPOS, F, 2 * P_SIZE), 1.0, 6.0, ((0, 32), (1, 8)), jnp.float32),
        "onset": set_ends(jax.random.randint(key_of[4], (NPOS, P_SIZE), NT // 8, NT - NT // 8), jax.random.fold_in(key_of[4], 1), NT // 8, (NT - NT // 8) - 1).astype(jnp.int32),
    }


def tables(freqs):
    samples = 2 * freqs
    order = lax.iota(jnp.int32, freqs)
    sample = lax.iota(jnp.int32, samples)
    phase = (order[:, None] * sample[None, :]) % samples
    phases = (2.0 * math.pi / samples) * phase.astype(jnp.float32)
    cosine = jnp.cos(phases)
    sine = jnp.sin(phases)
    factor = jnp.where(order == 0, 1.0, 2.0).astype(jnp.float32)[:, None] / samples
    inverse = jnp.stack([factor * cosine, -factor * sine])
    forward = jnp.stack([cosine, -sine])
    return inverse, forward, sample


def window(spectrum, onset):
    count, freqs, width = spectrum.shape
    half = width // 2
    inverse, forward, sample = tables(freqs)
    split = spectrum.reshape(count, freqs, 2, half)
    traces = jnp.einsum("nkcp,ckt->ntp", split, inverse, precision=lax.Precision.HIGHEST)
    keep = sample[None, :, None] < onset[:, None, :]
    clipped = jnp.where(keep, traces, 0.0)
    back = jnp.einsum("ntp,ckt->nkcp", clipped, forward, precision=lax.Precision.HIGHEST)
    return back.reshape(count, freqs, width)


def adjoint_terms(real_part, imag_part, values):
    half = values.shape[2] // 2
    first = jnp.einsum("frs,rfq->sfq", real_part, values, precision=lax.Precision.HIGHEST)
    second = jnp.einsum("frs,rfq->sfq", imag_part, values, precision=lax.Precision.HIGHEST)
    return jnp.concatenate([first[..., :half] + second[..., half:], first[..., half:] - second[..., :half]], axis=2)


def forward_terms(real_part, imag_part, values):
    half = values.shape[2] // 2
    first = jnp.einsum("frs,sfq->rfq", real_part, values, precision=lax.Precision.HIGHEST)
    second = jnp.einsum("frs,sfq->rfq", imag_part, values, precision=lax.Precision.HIGHEST)
    return jnp.concatenate([first[..., :half] - second[..., half:], first[..., half:] + second[..., :half]], axis=2)


def reference(response_real, response_imaginary, focus, initial, onset):
    adjoint = adjoint_terms(response_real, response_imaginary, focus)
    windowed = window(adjoint, onset)
    forward = forward_terms(response_real, response_imaginary, windowed)
    return initial - window(forward, onset)
```

```python
import functools
import heapq

import jax
import jax.numpy as jnp
import numpy as np
from jax import lax
from jax.experimental import pallas as pl
from jax.experimental.pallas import tpu as pltpu
from jax.sharding import PartitionSpec as P

MESH = pl.DeviceIdType.MESH
BF = jnp.bfloat16
F32 = jnp.float32

NF = 8
NZ, NY = 8, 4
FL = 12
ROWS = 48
SPLIT = 5
CHUNKS = ((0, 24), (24, 24))
RATE = 46.6e3
LATENCY = 1.8


def split(value):
    high = value.astype(BF)
    low = (value - high.astype(F32)).astype(BF)
    return high, low


def dft_tables(freqs):
    samples = 2 * freqs
    phase = np.arange(freqs)[:, None] * np.arange(samples)[None, :] % samples
    angle = 2.0 * np.pi / samples * phase
    cosine, sine = np.cos(angle), np.sin(angle)
    factor = np.where(np.arange(freqs) == 0, 1.0, 2.0)[:, None] / samples
    inverse = np.concatenate([factor * cosine, -factor * sine]).T
    forward = np.concatenate([cosine, -sine])
    out = []
    for table in (inverse, forward):
        table = table.astype(np.float32)
        high = table.astype(jnp.bfloat16)
        low = (table - high.astype(np.float32)).astype(jnp.bfloat16)
        out.append(np.concatenate([high, high, low], axis=1))
    return out


PARTS = {"a": (0, SPLIT), "b": (SPLIT, FL - SPLIT)}


def halves(part, sign):
    start, count = PARTS[part]
    first = (count + 1) // 2 if part == "a" else count // 2
    return (start, first) if sign > 0 else (start + first, count - first)


class Plan:
    def __init__(self):
        self.tasks = {}

    def add(self, name, deps, run, link=None, size=0, dur=0.1, rank=(0,)):
        self.tasks[name] = (tuple(deps), run, link, size, dur, rank)

    def order(self):
        free, arrived, done = {}, {}, {}
        left = dict(self.tasks)
        now, order = 0.0, []
        while left:
            ready, soonest = [], None
            for name, (deps, run, link, size, dur, rank) in left.items():
                when = 0.0
                for dep in deps:
                    when = max(when, arrived.get(dep, 1e9))
                if when <= now:
                    ready.append((rank, name))
                soonest = when if soonest is None else min(soonest, when)
            if not ready:
                if soonest >= 1e9:
                    raise ValueError("cycle")
                now = soonest
                continue
            _, name = min(ready)
            deps, run, link, size, dur, rank = left.pop(name)
            now += dur
            order.append(name)
            if link is None:
                arrived[name] = now
            else:
                start = max(now, free.get(link, 0.0))
                free[link] = start + size / RATE
                arrived[name] = free[link] + LATENCY
            done[name] = now
        self.finish = now
        self.times = arrived
        return order


def kernel(rr, ri, focus, onset, inv, fwd, out, *scratch):
    (part, stage_a1, stage_a2, stage_b1, stage_b2, gathered, xs, x1, y1, x2, y2, made, back,
     send_sem, recv_sem, win_send, win_recv, ret_send, ret_recv) = scratch
    me_f, me_r = lax.axis_index("freq"), lax.axis_index("rec")
    z, y = lax.div(me_r, NY), lax.rem(me_r, NY)

    def at_z(d):
        return lax.rem(z + (d + NZ), NZ) if d else z

    def at_y(d):
        return lax.rem(y + (d + NY), NY) if d else y

    def rec_of(dz, dy):
        return at_z(dz) * NY + at_y(dy)

    barrier = pltpu.get_barrier_semaphore()
    for dz, dy in ((1, 0), (-1, 0), (0, 1), (0, -1)):
        pl.semaphore_signal(barrier, inc=1, device_id=(me_f, rec_of(dz, dy)), device_id_type=MESH)
    for d in range(1, NF):
        pl.semaphore_signal(barrier, inc=1, device_id=(lax.rem(me_f + d, NF), me_r), device_id_type=MESH)
    pl.semaphore_wait(barrier, 4 + NF - 1)

    lane = lax.broadcasted_iota(jnp.int32, (ROWS, 128), 1)
    low_half = lane < 64
    plan = Plan()
    copies, waits = {}, []

    def piece(name, src, dst, target):
        index = len(copies)
        copies[name] = pltpu.make_async_remote_copy(
            src_ref=src, dst_ref=dst, send_sem=send_sem.at[index], recv_sem=recv_sem.at[index],
            device_id=(me_f, target), device_id_type=MESH)
        return copies[name]

    for f in range(FL):
        value = focus[:, f, :]
        turned = pltpu.roll(value, 64, 1)
        xs[f, 0:ROWS, :] = value
        xs[f, ROWS : 2 * ROWS, :] = jnp.where(low_half, turned, -turned)

    def adjoint(start, count):
        def run():
            def step(f, _):
                x_high, x_low = split(xs[f])
                both = jnp.concatenate([x_high, x_low], axis=1)
                for c in range(4):
                    cols = pl.ds(384 * c, 384)
                    high, low = split(jnp.concatenate([rr[f, :, cols], ri[f, :, cols]], axis=0))
                    dims = (((0,), (0,)), ((), ()))
                    one = lax.dot_general(high, both, dims, preferred_element_type=F32)
                    two = lax.dot_general(low, x_high, dims, preferred_element_type=F32)
                    total = one[:, :128] + one[:, 128:] + two
                    part[f, 2 * c : 2 * c + 2] = total.reshape(2, NY, ROWS, 128)
                return _

            lax.fori_loop(start, start + count, step, 0)

        return run

    for name, (start, count) in PARTS.items():
        plan.add("adj" + name, (), adjoint(start, count), dur=8.0 * count / FL, rank=(0, name != "b"))

    slot = {"a1": 0, "a2": 0, "b1": 0, "b2": 0}
    stages = {"a1": stage_a1, "a2": stage_a2, "b1": stage_b1, "b2": stage_b2}

    def staging(kind, count, nr):
        index = slot[kind]
        slot[kind] += 1
        return stages[kind].at[index, pl.ds(0, count), pl.ds(0, nr), :]

    def reduce_piece(name, kind, freqs, dz, dy, rows, target, adds, deps, link, rank):
        start, count = freqs
        r0, nr = rows
        src = part.at[pl.ds(start, count), at_z(dz), at_y(dy), pl.ds(r0, nr), :]
        dst = staging(kind, count, nr)
        copy = piece(name, src, dst, target)
        copies[name] = (copy, dst, start, count)

        def run():
            take(adds, dz, dy, rows)
            copy.start()

        plan.add(name, tuple(adds) + tuple(deps), run, link, count * nr * 512, 0.12, rank)

    def take(adds, dz, dy, rows):
        r0, nr = rows
        for other in adds:
            copy, dst, start, count = copies[other]
            copy.wait_recv()
            where = (pl.ds(start, count), at_z(dz), at_y(dy), pl.ds(r0, nr), slice(None))
            part[where] += dst[...]

    for h, rows in enumerate(CHUNKS):
        deep = NZ // 2
        order_y = (2, 1, -1, 0)
        order_z = (4, 3, -3, 2, -2, 1, -1, 0)
        both_y = {1: (2, 0), -1: (1, -1)}
        both_z = {1: (4, 2, -2, 0), -1: (3, -3, 1, -1)}
        for k in range(deep, 0, -1):
            for place, dy in enumerate(order_y):
                for sign in (1, -1):
                    if k == deep and dy not in both_y[sign]:
                        continue
                    adds = [f"a1{h},{sign},{k + 1},{dy}"] if (k < deep - 1 or (k == deep - 1 and dy in both_y[sign])) else []
                    reduce_piece(f"a1{h},{sign},{k},{dy}", "a1", PARTS["a"], sign * k, dy, rows, rec_of(sign, 0), adds,
                                 ("adja",), ("z", sign), (1, h, 0, -k, place))
        for k in (2, 1):
            for place, dz in enumerate(order_z):
                for sign in (1, -1):
                    if k == 2 and dz not in both_z[sign]:
                        continue
                    adds = [f"b1{h},{sign},2,{dz}"] if k == 1 and dz in both_z[sign] else []
                    reduce_piece(f"b1{h},{sign},{k},{dz}", "b1", PARTS["b"], dz, sign * k, rows, rec_of(0, sign), adds,
                                 ("adjb",), ("y", sign), (1, h, 0, -k, place))

        def first_sum(name, kind, d):
            keys = [f"{kind}{h},{sign},1,{d}" for sign in (1, -1)]

            def run(keys=keys, d=d, rows=rows, kind=kind):
                dz, dy = (0, d) if kind == "a1" else (d, 0)
                take(keys, dz, dy, rows)

            plan.add(name, keys, run, dur=0.12, rank=(0, h, 0))

        for dy in order_y:
            first_sum(f"as{h},{dy}", "a1", dy)
        for dz in order_z:
            first_sum(f"bs{h},{dz}", "b1", dz)
        for sign in (1, -1):
            reduce_piece(f"a2{h},{sign},2", "a2", halves("a", sign), 0, 2 * sign, rows, rec_of(0, sign), [],
                         (f"as{h},2",), ("y", sign), (0, h, 1, -2))
            reduce_piece(f"a2{h},{sign},1", "a2", PARTS["a"], 0, sign, rows, rec_of(0, sign), [f"a2{h},{sign},2"],
                         (f"as{h},{sign}",), ("y", sign), (0, h, 1, -1))
            for k in range(deep, 0, -1):
                freqs = halves("b", sign) if k == deep else PARTS["b"]
                adds = [] if k == deep else [f"b2{h},{sign},{k + 1}"]
                source = 4 if k == deep else sign * k
                reduce_piece(f"b2{h},{sign},{k}", "b2", freqs, sign * k, 0, rows, rec_of(sign, 0), adds,
                             (f"bs{h},{source}",), ("z", sign), (0, h, 1, -k))

        own_keys = [f"a2{h},{sign},1" for sign in (1, -1)] + [f"b2{h},{sign},1" for sign in (1, -1)]

        def own_sum(keys=tuple(own_keys), rows=rows):
            take(keys, 0, 0, rows)

        plan.add(f"own{h}", own_keys + [f"as{h},0", f"bs{h},0"], own_sum, dur=0.2, rank=(0, h, 0))

    def block_of(buffer, freqs, j):
        return buffer.at[freqs, z, y, pl.ds(8 * j, 8), :]

    def out_copy(source, landing, which, j):
        return pltpu.make_async_remote_copy(
            src_ref=source(j), dst_ref=landing.at[pl.ds(FL * me_f, FL)],
            send_sem=win_send.at[which, j], recv_sem=win_recv.at[which, me_f],
            device_id=(j, me_r), device_id_type=MESH)

    def in_wait(landing, which, sender):
        pltpu.make_async_remote_copy(
            src_ref=landing.at[pl.ds(FL * sender, FL)], dst_ref=landing.at[pl.ds(FL * sender, FL)],
            send_sem=win_send.at[which, 0], recv_sem=win_recv.at[which, sender],
            device_id=(sender, me_r), device_id_type=MESH).wait_recv()

    def return_copy(clipped, target, which, d):
        return pltpu.make_async_remote_copy(
            src_ref=clipped.at[pl.ds(FL * d, FL)], dst_ref=target(me_f),
            send_sem=ret_send.at[which, d], recv_sem=ret_recv.at[which, me_f],
            device_id=(d, me_r), device_id_type=MESH)

    def return_wait(target, which, j):
        pltpu.make_async_remote_copy(
            src_ref=target(j), dst_ref=target(j), send_sem=ret_send.at[which, 0],
            recv_sem=ret_recv.at[which, j], device_id=(j, me_r), device_id_type=MESH).wait_recv()

    def window(landing, clipped):
        half = lax.broadcasted_iota(jnp.int32, (NF * FL, 128), 1) < 64
        tops, bottoms = [], []
        for m in range(4):
            first, second = landing[:, 2 * m, :], landing[:, 2 * m + 1, :]
            tops.append(jnp.where(half, first, pltpu.roll(second, 64, 1)))
            bottoms.append(jnp.where(half, pltpu.roll(first, 64, 1), second))
        spectrum = jnp.concatenate([jnp.concatenate(tops, axis=1), jnp.concatenate(bottoms, axis=1)], axis=0)
        high, low = split(spectrum)
        traces = jnp.dot(inv[...], jnp.concatenate([high, low, high], axis=0), preferred_element_type=F32)
        limit = onset[jnp.minimum(me_f, ROWS // 8 - 1)]
        limits = jnp.concatenate([limit[m : m + 1, :] for m in range(4)], axis=1)
        sample = lax.broadcasted_iota(jnp.int32, traces.shape, 0)
        kept = jnp.where(sample < limits, traces, 0.0)
        high, low = split(kept)
        again = jnp.dot(fwd[...], jnp.concatenate([high, low, high], axis=0), preferred_element_type=F32)
        for m in range(4):
            real = again[: NF * FL, 128 * m : 128 * m + 128]
            imag = again[NF * FL :, 128 * m : 128 * m + 128]
            clipped[:, 2 * m, :] = jnp.where(half, real, pltpu.roll(imag, 64, 1))
            clipped[:, 2 * m + 1, :] = jnp.where(half, pltpu.roll(real, 64, 1), imag)

    def window_tasks(which, tag, members, source, landing, clipped, target, deps, rank):
        def scatter():
            for j in members:
                @pl.when(me_f != j)
                def _():
                    out_copy(source, landing, which, j).start()

                @pl.when(me_f == j)
                def _():
                    landing[FL * j : FL * j + FL] = source(j)[...]

        def apply():
            @pl.when((me_f >= members[0]) & (me_f <= members[-1]))
            def _():
                for sender in range(NF):
                    @pl.when(me_f != sender)
                    def _():
                        in_wait(landing, which, sender)

                window(landing, clipped)
                for d in range(NF):
                    @pl.when(me_f != d)
                    def _():
                        return_copy(clipped, target, which, d).start()

                target(me_f)[...] = clipped[pl.ds(FL * me_f, FL)]

        def collect():
            for j in members:
                @pl.when(me_f != j)
                def _():
                    return_wait(target, which, j)

        def drain():
            for j in members:
                @pl.when(me_f != j)
                def _():
                    out_copy(source, landing, which, j).wait_send()

            @pl.when((me_f >= members[0]) & (me_f <= members[-1]))
            def _():
                for d in range(NF):
                    @pl.when(me_f != d)
                    def _():
                        return_copy(clipped, target, which, d).wait_send()

        waits.append(drain)
        size = len(members) * 8 * FL * 512
        plan.add(tag + "out", deps, scatter, ("x", 0), size, 0.3, rank)
        plan.add(tag + "win", (tag + "out",), apply, ("x", 1), size, 1.5, rank)
        plan.add(tag + "in", (tag + "win",), collect, dur=0.2, rank=rank)

    everything = pl.ds(0, FL)
    for h, (r0, nr) in enumerate(CHUNKS):
        members = tuple(range(r0 // 8, (r0 + nr) // 8))
        window_tasks(0, f"w{h}", members, functools.partial(block_of, part, everything), x1, y1,
                     functools.partial(block_of, gathered, everything), (f"own{h}",), (0, h, 0))

    def gather_piece(name, freqs, dz, dy, rows, target, deps, link, rank):
        start, count = freqs
        r0, nr = rows
        where = gathered.at[pl.ds(start, count), at_z(dz), at_y(dy), pl.ds(r0, nr), :]
        copy = piece(name, where, where, target)
        arrivals = [dep for dep in deps if dep in copies]

        def run():
            for dep in arrivals:
                receive(dep)
            copy.start()

        plan.add(name, deps, run, link, count * nr * 512, 0.08, rank)

    received = set()

    def receive(name):
        if name not in received:
            received.add(name)
            copies[name].wait_recv()

    ends = {"a": [], "b": []}
    for h, rows in enumerate(CHUNKS):
        own = f"w{h}in"
        deep = NZ // 2
        for sign in (1, -1):
            gather_piece(f"ya{h},{sign},0", PARTS["a"], 0, 0, rows, rec_of(0, sign), (own,), ("y", sign), (2, h, 0))
            gather_piece(f"zb{h},{sign},0", PARTS["b"], 0, 0, rows, rec_of(sign, 0), (own,), ("z", sign), (2, h, 0))
        for sign in (1, -1):
            gather_piece(f"ya{h},{sign},1", halves("a", sign), 0, -sign, rows, rec_of(0, sign), (f"ya{h},{sign},0",),
                         ("y", sign), (2, h, 0))
            for k in range(1, deep):
                freqs = halves("b", sign) if k == deep - 1 else PARTS["b"]
                gather_piece(f"zb{h},{sign},{k}", freqs, -sign * k, 0, rows, rec_of(sign, 0), (f"zb{h},{sign},{k - 1}",),
                             ("z", sign), (2, h, 0))
        for dy in (0, -1, 1, 2):
            if dy == 0:
                deps = (own,)
            elif dy == 2:
                deps = (f"ya{h},1,1", f"ya{h},-1,1")
            else:
                deps = (f"ya{h},{-dy},0",)
            for sign in (1, -1):
                for k in range(deep):
                    if k == deep - 1 and dy not in both_y[sign]:
                        continue
                    gather_piece(f"za{h},{sign},{k},{dy}", PARTS["a"], -sign * k, dy, rows, rec_of(sign, 0),
                                 deps if k == 0 else (f"za{h},{sign},{k - 1},{dy}",), ("z", sign), (2, h, 1, k))
                    ends["a"].append(f"za{h},{sign},{k},{dy}")
        for dz in (0, -1, 1, -2, 2, -3, 3, 4):
            if dz == 0:
                deps = (own,)
            elif dz == 4:
                deps = (f"zb{h},1,{deep - 1}", f"zb{h},-1,{deep - 1}")
            else:
                sign = -1 if dz > 0 else 1
                deps = (f"zb{h},{sign},{abs(dz) - 1}",)
            for sign in (1, -1):
                for k in range(2):
                    if k == 1 and dz not in both_z[sign]:
                        continue
                    gather_piece(f"yb{h},{sign},{k},{dz}", PARTS["b"], dz, -sign * k, rows, rec_of(0, sign),
                                 deps if k == 0 else (f"yb{h},{sign},0,{dz}",), ("y", sign), (2, h, 1, k))
                    ends["b"].append(f"yb{h},{sign},{k},{dz}")
        for name in list(copies):
            if name.startswith((f"ya{h}", f"zb{h}")):
                ends[name[1]].append(name)

    def forward(name):
        start, count = PARTS[name]

        def run():
            for key in ends[name]:
                receive(key)

            def step(f, _):
                high, low = split(jnp.concatenate([rr[f], ri[f]], axis=0))
                w_high, w_low = split(gathered[f].reshape(NZ * NY * ROWS, 128))
                one = jnp.dot(high, jnp.concatenate([w_high, w_low], axis=1), preferred_element_type=F32)
                two = jnp.dot(low, w_high, preferred_element_type=F32)
                total = one[:, :128] + one[:, 128:] + two
                turned = pltpu.roll(total[ROWS:], 64, 1)
                made[f] = total[:ROWS] + jnp.where(low_half, -turned, turned)
                return _

            lax.fori_loop(start, start + count, step, 0)

        return run

    for name in PARTS:
        plan.add("fwd" + name, ends[name] + [f"w{h}in" for h in range(len(CHUNKS))], forward(name),
                 dur=6.0 * PARTS[name][1] / FL, rank=(3,))

    members = tuple(range(ROWS // 8))
    window_tasks(1, "v", members, lambda j: made.at[:, pl.ds(8 * j, 8), :], x2, y2,
                 lambda j: back.at[:, pl.ds(8 * j, 8), :], ("fwda", "fwdb"), (4,))

    order = plan.order()
    for name in order:
        plan.tasks[name][1]()
    out[...] = back[...]
    for value in copies.values():
        (value[0] if isinstance(value, tuple) else value).wait_send()
    for drain in waits:
        drain()
    kernel.plan = plan
    kernel.ordered = order


def iterate(response_real, response_imaginary, focus, onset, inv, fwd):
    chunks, nr = len(CHUNKS), CHUNKS[0][1]
    na, nb = SPLIT, FL - SPLIT
    vmem = pl.BlockSpec(memory_space=pltpu.VMEM)
    scratch = [
        pltpu.VMEM((FL, NZ, NY, ROWS, 128), F32),
        pltpu.VMEM((28 * chunks, na, nr, 128), F32),
        pltpu.VMEM((4 * chunks, na, nr, 128), F32),
        pltpu.VMEM((24 * chunks, nb, nr, 128), F32),
        pltpu.VMEM((8 * chunks, nb, nr, 128), F32),
        pltpu.VMEM((FL, NZ, NY, ROWS, 128), F32),
        pltpu.VMEM((FL, 2 * ROWS, 128), F32),
        pltpu.VMEM((NF * FL, 8, 128), F32),
        pltpu.VMEM((NF * FL, 8, 128), F32),
        pltpu.VMEM((NF * FL, 8, 128), F32),
        pltpu.VMEM((NF * FL, 8, 128), F32),
        pltpu.VMEM((FL, ROWS, 128), F32),
        pltpu.VMEM((FL, ROWS, 128), F32),
        pltpu.SemaphoreType.DMA((128 * chunks,)),
        pltpu.SemaphoreType.DMA((128 * chunks,)),
        pltpu.SemaphoreType.DMA((2, NF)),
        pltpu.SemaphoreType.DMA((2, NF)),
        pltpu.SemaphoreType.DMA((2, NF)),
        pltpu.SemaphoreType.DMA((2, NF)),
    ]
    return pl.pallas_call(
        kernel,
        out_shape=jax.ShapeDtypeStruct((FL, ROWS, 128), F32),
        in_specs=[vmem] * 6,
        out_specs=vmem,
        scratch_shapes=scratch,
        compiler_params=pltpu.CompilerParams(
            collective_id=0, has_side_effects=True, vmem_limit_bytes=60 * 1024 * 1024
        ),
    )(response_real, response_imaginary, focus, onset, inv, fwd)


def on_device(response_real, response_imaginary, focus, initial, onset):
    inv, fwd = dft_tables(NF * FL)
    pairs = onset.reshape(ROWS // 8, 4, 128)
    update = iterate(response_real, response_imaginary, focus, pairs, jnp.asarray(inv), jnp.asarray(fwd))
    return initial - jnp.transpose(update, (1, 0, 2))


def solution(mesh):
    in_specs = (
        P("freq", "rec", None),
        P("freq", "rec", None),
        P("rec", "freq", None),
        P("rec", "freq", None),
        P("rec", None),
    )
    return jax.shard_map(
        on_device, mesh=mesh, in_specs=in_specs, out_specs=P("rec", "freq", None), check_vma=False
    )
```

```python
import functools
import heapq

import jax
import jax.numpy as jnp
import numpy as np
from jax import lax
from jax.experimental import pallas as pl
from jax.experimental.pallas import tpu as pltpu
from jax.sharding import PartitionSpec as P

MESH = pl.DeviceIdType.MESH
BF = jnp.bfloat16
F32 = jnp.float32

NF = 8
NZ, NY = 8, 4
FL = 12
ROWS = 48
SPLIT = 5
CHUNKS = ((0, 24), (24, 24))
RATE = 46.6e3
LATENCY = 1.8
BACKLOG = 2.0


def split(value):
    high = value.astype(BF)
    low = (value - high.astype(F32)).astype(BF)
    return high, low


def dft_tables(freqs):
    samples = 2 * freqs
    phase = np.arange(freqs)[:, None] * np.arange(samples)[None, :] % samples
    angle = 2.0 * np.pi / samples * phase
    cosine, sine = np.cos(angle), np.sin(angle)
    factor = np.where(np.arange(freqs) == 0, 1.0, 2.0)[:, None] / samples
    inverse = np.concatenate([factor * cosine, -factor * sine]).T
    forward = np.concatenate([cosine, -sine])
    out = []
    for table in (inverse, forward):
        table = table.astype(np.float32)
        high = table.astype(jnp.bfloat16)
        low = (table - high.astype(np.float32)).astype(jnp.bfloat16)
        out.append(np.concatenate([high, high, low], axis=1))
    return out


PARTS = {"a": (0, SPLIT), "b": (SPLIT, FL - SPLIT)}


def halves(part, sign):
    start, count = PARTS[part]
    first = (count + 1) // 2 if part == "a" else count // 2
    return (start, first) if sign > 0 else (start + first, count - first)


class Plan:
    def __init__(self):
        self.tasks = {}

    def add(self, name, deps, run, link=None, size=0, dur=0.1, rank=(0,)):
        self.tasks[name] = (tuple(deps), run, link, size, dur, rank)

    def order(self):
        free, arrived, done = {}, {}, {}
        left = dict(self.tasks)
        now, order = 0.0, []
        while left:
            ready, soonest = [], None
            for name, (deps, run, link, size, dur, rank) in left.items():
                when = 0.0
                for dep in deps:
                    when = max(when, arrived.get(dep, 1e9))
                if link is not None:
                    when = max(when, free.get(link, 0.0) - BACKLOG)
                if when <= now:
                    ready.append((rank, name))
                soonest = when if soonest is None else min(soonest, when)
            if not ready:
                if soonest >= 1e9:
                    raise ValueError("cycle")
                now = soonest
                continue
            _, name = min(ready)
            deps, run, link, size, dur, rank = left.pop(name)
            now += dur
            order.append(name)
            if link is None:
                arrived[name] = now
            else:
                start = max(now, free.get(link, 0.0))
                free[link] = start + size / RATE
                arrived[name] = free[link] + LATENCY
            done[name] = now
        self.finish = now
        self.times = arrived
        return order


def kernel(rr, ri, focus, onset, inv, fwd, out, *scratch):
    (resp, load_sem, part, stage_a1, stage_a2, stage_b1, stage_b2, gathered, xs, x1, y1, x2, y2, made, back,
     send_sem, recv_sem, win_send, win_recv, ret_send, ret_recv) = scratch
    me_f, me_r = lax.axis_index("freq"), lax.axis_index("rec")
    z, y = lax.div(me_r, NY), lax.rem(me_r, NY)

    def at_z(d):
        return lax.rem(z + (d + NZ), NZ) if d else z

    def at_y(d):
        return lax.rem(y + (d + NY), NY) if d else y

    def rec_of(dz, dy):
        return at_z(dz) * NY + at_y(dy)

    def load(c, f):
        source = (rr, ri)[c]
        return pltpu.make_async_copy(source.at[f], resp.at[f, pl.ds(ROWS * c, ROWS), :], load_sem.at[c, f])

    for part_start, part_count in (PARTS["b"], PARTS["a"]):
        for f in range(part_start, part_start + part_count):
            load(0, f).start()
            load(1, f).start()

    barrier = pltpu.get_barrier_semaphore()
    for dz, dy in ((1, 0), (-1, 0), (0, 1), (0, -1)):
        pl.semaphore_signal(barrier, inc=1, device_id=(me_f, rec_of(dz, dy)), device_id_type=MESH)
    for d in range(1, NF):
        pl.semaphore_signal(barrier, inc=1, device_id=(lax.rem(me_f + d, NF), me_r), device_id_type=MESH)
    pl.semaphore_wait(barrier, 4 + NF - 1)

    lane = lax.broadcasted_iota(jnp.int32, (ROWS, 128), 1)
    low_half = lane < 64
    plan = Plan()
    copies, waits = {}, []

    def piece(name, src, dst, target):
        index = len(copies)
        copies[name] = pltpu.make_async_remote_copy(
            src_ref=src, dst_ref=dst, send_sem=send_sem.at[index], recv_sem=recv_sem.at[index],
            device_id=(me_f, target), device_id_type=MESH)
        return copies[name]

    for f in range(FL):
        value = focus[f]
        turned = pltpu.roll(value, 64, 1)
        xs[f, 0:ROWS, :] = value
        xs[f, ROWS : 2 * ROWS, :] = jnp.where(low_half, turned, -turned)

    def adjoint(start, count):
        def run():
            def step(f, _):
                load(0, f).wait()
                load(1, f).wait()
                x_high, x_low = split(xs[f])
                both = jnp.concatenate([x_high, x_low], axis=1)
                for c in range(4):
                    cols = pl.ds(384 * c, 384)
                    high, low = split(resp[f, :, cols])
                    dims = (((0,), (0,)), ((), ()))
                    one = lax.dot_general(high, both, dims, preferred_element_type=F32)
                    two = lax.dot_general(low, x_high, dims, preferred_element_type=F32)
                    total = one[:, :128] + one[:, 128:] + two
                    part[f, 2 * c : 2 * c + 2] = total.reshape(2, NY, ROWS, 128)
                return _

            lax.fori_loop(start, start + count, step, 0)

        return run

    for name, (start, count) in PARTS.items():
        plan.add("adj" + name, (), adjoint(start, count), dur=8.0 * count / FL, rank=(0, name != "b"))

    slot = {"a1": 0, "a2": 0, "b1": 0, "b2": 0}
    stages = {"a1": stage_a1, "a2": stage_a2, "b1": stage_b1, "b2": stage_b2}

    def staging(kind, count, nr):
        index = slot[kind]
        slot[kind] += 1
        return stages[kind].at[index, pl.ds(0, count), pl.ds(0, nr), :]

    def reduce_piece(name, kind, freqs, dz, dy, rows, target, adds, deps, link, rank):
        start, count = freqs
        r0, nr = rows
        src = part.at[pl.ds(start, count), at_z(dz), at_y(dy), pl.ds(r0, nr), :]
        dst = staging(kind, count, nr)
        copy = piece(name, src, dst, target)
        copies[name] = (copy, dst, start, count)

        def run():
            take(adds, dz, dy, rows)
            copy.start()

        plan.add(name, tuple(adds) + tuple(deps), run, link, count * nr * 512, 0.12, rank)

    def take(adds, dz, dy, rows):
        r0, nr = rows
        for other in adds:
            copy, dst, start, count = copies[other]
            copy.wait_recv()
            where = (pl.ds(start, count), at_z(dz), at_y(dy), pl.ds(r0, nr), slice(None))
            part[where] += dst[...]

    for h, rows in enumerate(CHUNKS):
        deep = NZ // 2
        order_y = (2, 1, -1, 0)
        order_z = (4, 3, -3, 2, -2, 1, -1, 0)
        both_y = {1: (2, 0), -1: (1, -1)}
        both_z = {1: (4, 2, -2, 0), -1: (3, -3, 1, -1)}
        for k in range(deep, 0, -1):
            for place, dy in enumerate(order_y):
                for sign in (1, -1):
                    if k == deep and dy not in both_y[sign]:
                        continue
                    adds = [f"a1{h},{sign},{k + 1},{dy}"] if (k < deep - 1 or (k == deep - 1 and dy in both_y[sign])) else []
                    reduce_piece(f"a1{h},{sign},{k},{dy}", "a1", PARTS["a"], sign * k, dy, rows, rec_of(sign, 0), adds,
                                 ("adja",), ("z", sign), (1, h, 0, -k, place))
        for k in (2, 1):
            for place, dz in enumerate(order_z):
                for sign in (1, -1):
                    if k == 2 and dz not in both_z[sign]:
                        continue
                    adds = [f"b1{h},{sign},2,{dz}"] if k == 1 and dz in both_z[sign] else []
                    reduce_piece(f"b1{h},{sign},{k},{dz}", "b1", PARTS["b"], dz, sign * k, rows, rec_of(0, sign), adds,
                                 ("adjb",), ("y", sign), (1, h, 0, -k, place))

        def first_sum(name, kind, d):
            keys = [f"{kind}{h},{sign},1,{d}" for sign in (1, -1)]

            def run(keys=keys, d=d, rows=rows, kind=kind):
                dz, dy = (0, d) if kind == "a1" else (d, 0)
                take(keys, dz, dy, rows)

            plan.add(name, keys, run, dur=0.12, rank=(0, h, 0))

        for dy in order_y:
            first_sum(f"as{h},{dy}", "a1", dy)
        for dz in order_z:
            first_sum(f"bs{h},{dz}", "b1", dz)
        for sign in (1, -1):
            reduce_piece(f"a2{h},{sign},2", "a2", halves("a", sign), 0, 2 * sign, rows, rec_of(0, sign), [],
                         (f"as{h},2",), ("y", sign), (0, h, 1, -2))
            reduce_piece(f"a2{h},{sign},1", "a2", PARTS["a"], 0, sign, rows, rec_of(0, sign), [f"a2{h},{sign},2"],
                         (f"as{h},{sign}",), ("y", sign), (0, h, 1, -1))
            for k in range(deep, 0, -1):
                freqs = halves("b", sign) if k == deep else PARTS["b"]
                adds = [] if k == deep else [f"b2{h},{sign},{k + 1}"]
                source = 4 if k == deep else sign * k
                reduce_piece(f"b2{h},{sign},{k}", "b2", freqs, sign * k, 0, rows, rec_of(sign, 0), adds,
                             (f"bs{h},{source}",), ("z", sign), (0, h, 1, -k))

        own_keys = [f"a2{h},{sign},1" for sign in (1, -1)] + [f"b2{h},{sign},1" for sign in (1, -1)]

        def own_sum(keys=tuple(own_keys), rows=rows):
            take(keys, 0, 0, rows)

        plan.add(f"own{h}", own_keys + [f"as{h},0", f"bs{h},0"], own_sum, dur=0.2, rank=(0, h, 0))

    def block_of(buffer, freqs, j):
        return buffer.at[freqs, z, y, pl.ds(8 * j, 8), :]

    def out_copy(source, landing, which, j):
        return pltpu.make_async_remote_copy(
            src_ref=source(j), dst_ref=landing.at[pl.ds(FL * me_f, FL)],
            send_sem=win_send.at[which, j], recv_sem=win_recv.at[which, me_f],
            device_id=(j, me_r), device_id_type=MESH)

    def in_wait(landing, which, sender):
        pltpu.make_async_remote_copy(
            src_ref=landing.at[pl.ds(FL * sender, FL)], dst_ref=landing.at[pl.ds(FL * sender, FL)],
            send_sem=win_send.at[which, 0], recv_sem=win_recv.at[which, sender],
            device_id=(sender, me_r), device_id_type=MESH).wait_recv()

    def return_copy(clipped, target, which, d):
        return pltpu.make_async_remote_copy(
            src_ref=clipped.at[pl.ds(FL * d, FL)], dst_ref=target(me_f),
            send_sem=ret_send.at[which, d], recv_sem=ret_recv.at[which, me_f],
            device_id=(d, me_r), device_id_type=MESH)

    def return_wait(target, which, j):
        pltpu.make_async_remote_copy(
            src_ref=target(j), dst_ref=target(j), send_sem=ret_send.at[which, 0],
            recv_sem=ret_recv.at[which, j], device_id=(j, me_r), device_id_type=MESH).wait_recv()

    def window(landing, clipped):
        half = lax.broadcasted_iota(jnp.int32, (NF * FL, 128), 1) < 64
        tops, bottoms = [], []
        for m in range(4):
            first, second = landing[:, 2 * m, :], landing[:, 2 * m + 1, :]
            tops.append(jnp.where(half, first, pltpu.roll(second, 64, 1)))
            bottoms.append(jnp.where(half, pltpu.roll(first, 64, 1), second))
        spectrum = jnp.concatenate([jnp.concatenate(tops, axis=1), jnp.concatenate(bottoms, axis=1)], axis=0)
        high, low = split(spectrum)
        traces = jnp.dot(inv[...], jnp.concatenate([high, low, high], axis=0), preferred_element_type=F32)
        limit = onset[pl.ds(pl.multiple_of(8 * jnp.minimum(me_f, ROWS // 8 - 1), 8), 8), :]
        limits = jnp.concatenate([limit[m : m + 1, :] for m in range(8)], axis=1)
        sample = lax.broadcasted_iota(jnp.int32, traces.shape, 0)
        kept = jnp.where(sample < limits, traces, 0.0)
        high, low = split(kept)
        again = jnp.dot(fwd[...], jnp.concatenate([high, low, high], axis=0), preferred_element_type=F32)
        for m in range(4):
            real = again[: NF * FL, 128 * m : 128 * m + 128]
            imag = again[NF * FL :, 128 * m : 128 * m + 128]
            clipped[:, 2 * m, :] = jnp.where(half, real, pltpu.roll(imag, 64, 1))
            clipped[:, 2 * m + 1, :] = jnp.where(half, pltpu.roll(real, 64, 1), imag)

    def window_tasks(which, tag, members, source, landing, clipped, target, deps, rank):
        def scatter():
            for j in members:
                @pl.when(me_f != j)
                def _():
                    out_copy(source, landing, which, j).start()

                @pl.when(me_f == j)
                def _():
                    landing[FL * j : FL * j + FL] = source(j)[...]

        def apply():
            @pl.when((me_f >= members[0]) & (me_f <= members[-1]))
            def _():
                for sender in range(NF):
                    @pl.when(me_f != sender)
                    def _():
                        in_wait(landing, which, sender)

                window(landing, clipped)
                for d in range(NF):
                    @pl.when(me_f != d)
                    def _():
                        return_copy(clipped, target, which, d).start()

                target(me_f)[...] = clipped[pl.ds(FL * me_f, FL)]

        def collect():
            for j in members:
                @pl.when(me_f != j)
                def _():
                    return_wait(target, which, j)

        def drain():
            for j in members:
                @pl.when(me_f != j)
                def _():
                    out_copy(source, landing, which, j).wait_send()

            @pl.when((me_f >= members[0]) & (me_f <= members[-1]))
            def _():
                for d in range(NF):
                    @pl.when(me_f != d)
                    def _():
                        return_copy(clipped, target, which, d).wait_send()

        waits.append(drain)
        size = len(members) * 8 * FL * 512
        plan.add(tag + "out", deps, scatter, ("x", 0), size, 0.3, rank)
        plan.add(tag + "win", (tag + "out",), apply, ("x", 1), size, 1.5, rank)
        plan.add(tag + "in", (tag + "win",), collect, dur=0.2, rank=rank)

    everything = pl.ds(0, FL)
    for h, (r0, nr) in enumerate(CHUNKS):
        members = tuple(range(r0 // 8, (r0 + nr) // 8))
        window_tasks(0, f"w{h}", members, functools.partial(block_of, part, everything), x1, y1,
                     functools.partial(block_of, gathered, everything), (f"own{h}",), (0, h, 0))

    def gather_piece(name, freqs, dz, dy, rows, target, deps, link, rank):
        start, count = freqs
        r0, nr = rows
        where = gathered.at[pl.ds(start, count), at_z(dz), at_y(dy), pl.ds(r0, nr), :]
        copy = piece(name, where, where, target)
        arrivals = [dep for dep in deps if dep in copies]

        def run():
            for dep in arrivals:
                receive(dep)
            copy.start()

        plan.add(name, deps, run, link, count * nr * 512, 0.08, rank)

    received = set()

    def receive(name):
        if name not in received:
            received.add(name)
            copies[name].wait_recv()

    ends = {"a": [], "b": []}
    for h, rows in enumerate(CHUNKS):
        own = f"w{h}in"
        deep = NZ // 2
        for sign in (1, -1):
            gather_piece(f"ya{h},{sign},0", PARTS["a"], 0, 0, rows, rec_of(0, sign), (own,), ("y", sign), (2, h, 0))
            gather_piece(f"zb{h},{sign},0", PARTS["b"], 0, 0, rows, rec_of(sign, 0), (own,), ("z", sign), (2, h, 0))
        for sign in (1, -1):
            gather_piece(f"ya{h},{sign},1", halves("a", sign), 0, -sign, rows, rec_of(0, sign), (f"ya{h},{sign},0",),
                         ("y", sign), (2, h, 0))
            for k in range(1, deep):
                freqs = halves("b", sign) if k == deep - 1 else PARTS["b"]
                gather_piece(f"zb{h},{sign},{k}", freqs, -sign * k, 0, rows, rec_of(sign, 0), (f"zb{h},{sign},{k - 1}",),
                             ("z", sign), (2, h, 0))
        for dy in (0, -1, 1, 2):
            if dy == 0:
                deps = (own,)
            elif dy == 2:
                deps = (f"ya{h},1,1", f"ya{h},-1,1")
            else:
                deps = (f"ya{h},{-dy},0",)
            for sign in (1, -1):
                for k in range(deep):
                    if k == deep - 1 and dy not in both_y[sign]:
                        continue
                    gather_piece(f"za{h},{sign},{k},{dy}", PARTS["a"], -sign * k, dy, rows, rec_of(sign, 0),
                                 deps if k == 0 else (f"za{h},{sign},{k - 1},{dy}",), ("z", sign), (2, h, 1, k))
                    ends["a"].append(f"za{h},{sign},{k},{dy}")
        for dz in (0, -1, 1, -2, 2, -3, 3, 4):
            if dz == 0:
                deps = (own,)
            elif dz == 4:
                deps = (f"zb{h},1,{deep - 1}", f"zb{h},-1,{deep - 1}")
            else:
                sign = -1 if dz > 0 else 1
                deps = (f"zb{h},{sign},{abs(dz) - 1}",)
            for sign in (1, -1):
                for k in range(2):
                    if k == 1 and dz not in both_z[sign]:
                        continue
                    gather_piece(f"yb{h},{sign},{k},{dz}", PARTS["b"], dz, -sign * k, rows, rec_of(0, sign),
                                 deps if k == 0 else (f"yb{h},{sign},0,{dz}",), ("y", sign), (2, h, 1, k))
                    ends["b"].append(f"yb{h},{sign},{k},{dz}")
        for name in list(copies):
            if name.startswith((f"ya{h}", f"zb{h}")):
                ends[name[1]].append(name)

    def forward(name):
        start, count = PARTS[name]

        def run():
            for key in ends[name]:
                receive(key)

            def step(f, _):
                high, low = split(resp[f])
                w_high, w_low = split(gathered[f].reshape(NZ * NY * ROWS, 128))
                one = jnp.dot(high, jnp.concatenate([w_high, w_low], axis=1), preferred_element_type=F32)
                two = jnp.dot(low, w_high, preferred_element_type=F32)
                total = one[:, :128] + one[:, 128:] + two
                turned = pltpu.roll(total[ROWS:], 64, 1)
                made[f] = total[:ROWS] + jnp.where(low_half, -turned, turned)
                return _

            lax.fori_loop(start, start + count, step, 0)

        return run

    for name in PARTS:
        plan.add("fwd" + name, ends[name] + [f"w{h}in" for h in range(len(CHUNKS))], forward(name),
                 dur=6.0 * PARTS[name][1] / FL, rank=(3,))

    members = tuple(range(ROWS // 8))
    window_tasks(1, "v", members, lambda j: made.at[:, pl.ds(8 * j, 8), :], x2, y2,
                 lambda j: back.at[:, pl.ds(8 * j, 8), :], ("fwda", "fwdb"), (4,))

    order = plan.order()
    for name in order:
        plan.tasks[name][1]()
    out[...] = back[...]
    for value in copies.values():
        (value[0] if isinstance(value, tuple) else value).wait_send()
    for drain in waits:
        drain()
    kernel.plan = plan
    kernel.ordered = order


def iterate(response_real, response_imaginary, focus, onset, inv, fwd):
    chunks, nr = len(CHUNKS), CHUNKS[0][1]
    na, nb = SPLIT, FL - SPLIT
    vmem = pl.BlockSpec(memory_space=pltpu.VMEM)
    scratch = [
        pltpu.VMEM((FL, 2 * ROWS, response_real.shape[2]), F32),
        pltpu.SemaphoreType.DMA((2, FL)),
        pltpu.VMEM((FL, NZ, NY, ROWS, 128), F32),
        pltpu.VMEM((28 * chunks, na, nr, 128), F32),
        pltpu.VMEM((4 * chunks, na, nr, 128), F32),
        pltpu.VMEM((24 * chunks, nb, nr, 128), F32),
        pltpu.VMEM((8 * chunks, nb, nr, 128), F32),
        pltpu.VMEM((FL, NZ, NY, ROWS, 128), F32),
        pltpu.VMEM((FL, 2 * ROWS, 128), F32),
        pltpu.VMEM((NF * FL, 8, 128), F32),
        pltpu.VMEM((NF * FL, 8, 128), F32),
        pltpu.VMEM((NF * FL, 8, 128), F32),
        pltpu.VMEM((NF * FL, 8, 128), F32),
        pltpu.VMEM((FL, ROWS, 128), F32),
        pltpu.VMEM((FL, ROWS, 128), F32),
        pltpu.SemaphoreType.DMA((128 * chunks,)),
        pltpu.SemaphoreType.DMA((128 * chunks,)),
        pltpu.SemaphoreType.DMA((2, NF)),
        pltpu.SemaphoreType.DMA((2, NF)),
        pltpu.SemaphoreType.DMA((2, NF)),
        pltpu.SemaphoreType.DMA((2, NF)),
    ]
    return pl.pallas_call(
        kernel,
        out_shape=jax.ShapeDtypeStruct((FL, ROWS, 128), F32),
        in_specs=[pl.BlockSpec(memory_space=pl.ANY)] * 2 + [vmem] * 4,
        out_specs=vmem,
        scratch_shapes=scratch,
        compiler_params=pltpu.CompilerParams(
            collective_id=0, has_side_effects=True, vmem_limit_bytes=60 * 1024 * 1024
        ),
    )(response_real, response_imaginary, focus, onset, inv, fwd)


def on_device(response_real, response_imaginary, focus, initial, onset):
    inv, fwd = dft_tables(NF * FL)
    by_freq = jnp.transpose(focus, (1, 0, 2))
    update = iterate(response_real, response_imaginary, by_freq, onset, jnp.asarray(inv), jnp.asarray(fwd))
    return initial - jnp.transpose(update, (1, 0, 2))


def solution(mesh):
    in_specs = (
        P("freq", "rec", None),
        P("freq", "rec", None),
        P("rec", "freq", None),
        P("rec", "freq", None),
        P("rec", None),
    )
    return jax.shard_map(
        on_device, mesh=mesh, in_specs=in_specs, out_specs=P("rec", "freq", None), check_vma=False
    )
```

```python
import functools
import heapq

import jax
import jax.numpy as jnp
import numpy as np
from jax import lax
from jax.experimental import pallas as pl
from jax.experimental.pallas import tpu as pltpu
from jax.sharding import PartitionSpec as P

MESH = pl.DeviceIdType.MESH
BF = jnp.bfloat16
F32 = jnp.float32

NF = 8
NZ, NY = 8, 4
FL = 12
ROWS = 48
SPLIT = 5
CHUNKS = 2
NR = ROWS // CHUNKS
COLS = NZ * NY * NR
MEMBERS = NR // 8
RATE = 46.6e3
LATENCY = 1.8
BACKLOG = 2.0


def split(value):
    high = value.astype(BF)
    low = (value - high.astype(F32)).astype(BF)
    return high, low


def dft_tables(freqs):
    samples = 2 * freqs
    phase = np.arange(freqs)[:, None] * np.arange(samples)[None, :] % samples
    angle = 2.0 * np.pi / samples * phase
    cosine, sine = np.cos(angle), np.sin(angle)
    factor = np.where(np.arange(freqs) == 0, 1.0, 2.0)[:, None] / samples
    inverse = np.concatenate([factor * cosine, -factor * sine]).T
    forward = np.concatenate([cosine, -sine])
    out = []
    for table in (inverse, forward):
        table = table.astype(np.float32)
        high = table.astype(jnp.bfloat16)
        low = (table - high.astype(np.float32)).astype(jnp.bfloat16)
        out.append(np.concatenate([high, high, low], axis=1))
    return out


PARTS = {"a": (0, SPLIT), "b": (SPLIT, FL - SPLIT)}


def halves(part, sign):
    start, count = PARTS[part]
    first = (count + 1) // 2 if part == "a" else count // 2
    return (start, first) if sign > 0 else (start + first, count - first)


class Plan:
    def __init__(self):
        self.tasks, self.sent = {}, {}

    def add(self, name, deps, run, link=None, size=0, dur=0.1, rank=(0,)):
        self.tasks[name] = (tuple(deps), run, link, size, dur, rank)

    def order(self):
        free, arrived, done = {}, {}, {}
        left = dict(self.tasks)
        now, order = 0.0, []
        while left:
            ready, soonest = [], None
            for name, (deps, run, link, size, dur, rank) in left.items():
                when = 0.0
                for dep in deps:
                    when = max(when, arrived.get(dep, 1e9))
                if link is not None:
                    when = max(when, free.get(link, 0.0) - BACKLOG)
                if when <= now:
                    ready.append((rank, name))
                soonest = when if soonest is None else min(soonest, when)
            if not ready:
                if soonest >= 1e9:
                    raise ValueError("cycle")
                now = soonest
                continue
            _, name = min(ready)
            deps, run, link, size, dur, rank = left.pop(name)
            now += dur
            order.append((now, name))
            if link is None:
                arrived[name] = now
            else:
                start = max(now, free.get(link, 0.0))
                free[link] = start + size / RATE
                arrived[name] = free[link] + LATENCY
                self.sent[name] = free[link]
            done[name] = now
        self.finish = now
        self.times = arrived
        return order


def kernel(rr, ri, focus_in, onset_in, inv_in, fwd_in, out, *scratch):
    (focus, onset, inv, fwd, small_sem, resp, load_sem, part, stage_a1, stage_a2, stage_b1, stage_b2, gathered, xs, x1, y1, x2, y2, acc, made, back,
     onset_own, onset_send, onset_recv, send_sem, recv_sem, win_send, win_recv, ret_send, ret_recv) = scratch
    me_f, me_r = lax.axis_index("freq"), lax.axis_index("rec")
    z, y = lax.div(me_r, NY), lax.rem(me_r, NY)

    def at_z(d):
        return lax.rem(z + (d + NZ), NZ) if d else z

    def at_y(d):
        return lax.rem(y + (d + NY), NY) if d else y

    def rec_of(dz, dy):
        return at_z(dz) * NY + at_y(dy)

    def load(c, h, name):
        start, count = PARTS[name]
        cols, freqs = pl.ds(COLS * h, COLS), pl.ds(start, count)
        return pltpu.make_async_copy(
            (rr, ri)[c].at[freqs, :, cols], resp.at[freqs, pl.ds(ROWS * c, ROWS), cols],
            load_sem.at[c, h, list(PARTS).index(name)])

    small = [pltpu.make_async_copy(src, dst, small_sem.at[i]) for i, (src, dst) in enumerate(
        ((focus_in, focus), (onset_in, onset), (inv_in, inv), (fwd_in, fwd)))]
    small[0].start()
    for h in range(CHUNKS):
        for name in PARTS:
            load(0, h, name).start()
            load(1, h, name).start()
        if h == 0:
            for copy in small[1:]:
                copy.start()

    barrier = pltpu.get_barrier_semaphore()
    for dz, dy in ((1, 0), (-1, 0), (0, 1), (0, -1)):
        pl.semaphore_signal(barrier, inc=1, device_id=(me_f, rec_of(dz, dy)), device_id_type=MESH)
    for d in range(1, NF):
        pl.semaphore_signal(barrier, inc=1, device_id=(lax.rem(me_f + d, NF), me_r), device_id_type=MESH)

    def onset_source(h):
        return lax.div(h * NZ * NY + me_r, CHUNKS)

    def onset_copy(u):
        index = me_r * CHUNKS + u
        target, h = lax.rem(index, NZ * NY), lax.div(index, NZ * NY)
        rows = onset.at[pl.ds(NR * u, NR), :]
        return target, h, rows, pltpu.make_async_remote_copy(
            src_ref=rows, dst_ref=onset_own.at[h], send_sem=onset_send.at[u], recv_sem=onset_recv.at[h],
            device_id=(me_f, target), device_id_type=MESH)

    for h in range(CHUNKS):
        @pl.when(onset_source(h) != me_r)
        def _():
            pl.semaphore_signal(barrier, inc=1, device_id=(me_f, onset_source(h)), device_id_type=MESH)

    def enter():
        for copy in small[1:]:
            copy.wait()
        peers = 4 + NF - 1
        for u in range(CHUNKS):
            peers += jnp.where(lax.rem(me_r * CHUNKS + u, NZ * NY) != me_r, 1, 0)
        pl.semaphore_wait(barrier, peers)
        for u in range(CHUNKS):
            target, h, rows, copy = onset_copy(u)

            @pl.when(target != me_r)
            def _():
                copy.start()

            @pl.when(target == me_r)
            def _():
                onset_own[h] = rows[...]

    def onset_ready():
        for u in range(CHUNKS):
            target, _h, _rows, copy = onset_copy(u)

            @pl.when(target != me_r)
            def _():
                copy.wait_send()

        for h in range(CHUNKS):
            @pl.when(onset_source(h) != me_r)
            def _():
                pltpu.make_async_remote_copy(
                    src_ref=onset_own.at[h], dst_ref=onset_own.at[h], send_sem=onset_send.at[0],
                    recv_sem=onset_recv.at[h], device_id=(me_f, me_r), device_id_type=MESH).wait_recv()

    lane = lax.broadcasted_iota(jnp.int32, (ROWS, 128), 1)
    low_half = lane < 64
    plan = Plan()
    copies = {}

    used = {}

    def piece(name, src, dst, target, phase, h):
        bank = h if phase == 0 else (CHUNKS + h if h < CHUNKS - 1 else 0)
        index = used[phase, h] = used.get((phase, h), -1) + 1
        copies[name] = pltpu.make_async_remote_copy(
            src_ref=src, dst_ref=dst, send_sem=send_sem.at[phase], recv_sem=recv_sem.at[bank, index],
            device_id=(me_f, target), device_id_type=MESH)
        return copies[name]

    small[0].wait()
    for f in range(FL):
        value = focus[f]
        turned = pltpu.roll(value, 64, 1)
        xs[f, 0:ROWS, :] = value
        xs[f, ROWS : 2 * ROWS, :] = jnp.where(low_half, turned, -turned)

    def adjoint(freqs, h, name):
        def run():
            if freqs[0] == PARTS[name][0]:
                load(0, h, name).wait()
                load(1, h, name).wait()

            def step(f, _):
                x_high, x_low = split(xs[f])
                left = jnp.concatenate([x_high, x_high], axis=0)
                right = jnp.concatenate([x_low, jnp.zeros_like(x_low)], axis=0)
                both = jnp.concatenate([left, right], axis=1)
                for c in range(2):
                    high, low = split(resp[f, :, pl.ds(COLS * h + COLS // 2 * c, COLS // 2)])
                    terms = lax.dot_general(jnp.concatenate([high, low], axis=0), both, (((0,), (0,)), ((), ())),
                                            preferred_element_type=F32)
                    total = terms[:, :128] + terms[:, 128:]
                    part[f, h, NZ // 2 * c : NZ // 2 * (c + 1)] = total.reshape(NZ // 2, NY, NR, 128)
                return _

            for f in freqs:
                step(f, 0)

        return run

    def groups(name, size):
        start, count = PARTS[name]
        return [tuple(range(f, min(f + size, start + count))) for f in range(start, start + count, size)]

    adjoint_done = {}
    for h in range(CHUNKS):
        for name in ("a", "b"):
            adjoint_done[h, name] = []
            for place, freqs in enumerate(groups(name, FL if h == 0 else 3)):
                key = f"adj{name}{h},{place}"
                adjoint_done[h, name].append(key)
                plan.add(key, (), adjoint(freqs, h, name), dur=3.4 / CHUNKS * len(freqs) / FL, rank=(0 if h == 0 else 1, max(h - 1, 0), 9, name != "a", place))

    slot = {"a1": 0, "a2": 0, "b1": 0, "b2": 0}
    stages = {"a1": stage_a1, "a2": stage_a2, "b1": stage_b1, "b2": stage_b2}

    def staging(kind, count):
        index = slot[kind]
        slot[kind] += 1
        return stages[kind].at[index, pl.ds(0, count)]

    def reduce_piece(name, kind, freqs, dz, dy, h, target, adds, deps, link, rank):
        start, count = freqs
        src = part.at[pl.ds(start, count), h, at_z(dz), at_y(dy)]
        dst = staging(kind, count)
        copy = piece(name, src, dst, target, 0, h)
        copies[name] = (copy, dst, start, count)

        def run():
            take(adds, dz, dy, h)
            copy.start()

        plan.add(name, tuple(adds) + tuple(deps), run, link, count * NR * 512, 0.12, rank)

    def take(adds, dz, dy, h):
        for other in adds:
            copy, dst, start, count = copies[other]
            copy.wait_recv()
            where = (pl.ds(start, count), h, at_z(dz), at_y(dy))
            part[where] += dst[...]

    for h in range(CHUNKS):
        deep = NZ // 2
        order_y = (2, 1, -1, 0)
        order_z = (4, 3, -3, 2, -2, 1, -1, 0)
        both_y = {1: (2, 0), -1: (1, -1)}
        both_z = {1: (4, 2, -2, 0), -1: (3, -3, 1, -1)}
        for k in range(deep, 0, -1):
            for place, dy in enumerate(order_y):
                for sign in (1, -1):
                    if k == deep and dy not in both_y[sign]:
                        continue
                    adds = [f"a1{h},{sign},{k + 1},{dy}"] if (k < deep - 1 or (k == deep - 1 and dy in both_y[sign])) else []
                    reduce_piece(f"a1{h},{sign},{k},{dy}", "a1", PARTS["a"], sign * k, dy, h, rec_of(sign, 0), adds,
                                 adjoint_done[h, "a"], ("z", sign), (1, h, 0, -k, place))
        for k in (2, 1):
            for place, dz in enumerate(order_z):
                for sign in (1, -1):
                    if k == 2 and dz not in both_z[sign]:
                        continue
                    adds = [f"b1{h},{sign},2,{dz}"] if k == 1 and dz in both_z[sign] else []
                    reduce_piece(f"b1{h},{sign},{k},{dz}", "b1", PARTS["b"], dz, sign * k, h, rec_of(0, sign), adds,
                                 adjoint_done[h, "b"], ("y", sign), (1, h, 0, -k, place))

        def first_sum(name, kind, d):
            keys = [f"{kind}{h},{sign},1,{d}" for sign in (1, -1)]

            def run(keys=keys, d=d, h=h, kind=kind):
                dz, dy = (0, d) if kind == "a1" else (d, 0)
                take(keys, dz, dy, h)

            plan.add(name, keys, run, dur=0.12, rank=(0, h, 0))

        for dy in order_y:
            first_sum(f"as{h},{dy}", "a1", dy)
        for dz in order_z:
            first_sum(f"bs{h},{dz}", "b1", dz)
        for sign in (1, -1):
            reduce_piece(f"a2{h},{sign},2", "a2", halves("a", sign), 0, 2 * sign, h, rec_of(0, sign), [],
                         (f"as{h},2",), ("y", sign), (0, h, 1, -2))
            reduce_piece(f"a2{h},{sign},1", "a2", PARTS["a"], 0, sign, h, rec_of(0, sign), [f"a2{h},{sign},2"],
                         (f"as{h},{sign}",), ("y", sign), (0, h, 1, -1))
            for k in range(deep, 0, -1):
                freqs = halves("b", sign) if k == deep else PARTS["b"]
                adds = [] if k == deep else [f"b2{h},{sign},{k + 1}"]
                source = 4 if k == deep else sign * k
                reduce_piece(f"b2{h},{sign},{k}", "b2", freqs, sign * k, 0, h, rec_of(sign, 0), adds,
                             (f"bs{h},{source}",), ("z", sign), (0, h, 1, -k))

        own_keys = [f"a2{h},{sign},1" for sign in (1, -1)] + [f"b2{h},{sign},1" for sign in (1, -1)]

        def own_sum(keys=tuple(own_keys), h=h):
            take(keys, 0, 0, h)

        plan.add(f"own{h}", own_keys + [f"as{h},0", f"bs{h},0"], own_sum, dur=0.2, rank=(0, h, 0))

    def block_of(buffer, h, j):
        return buffer.at[:, h, z, y, pl.ds(8 * (j - MEMBERS * h), 8), :]

    def out_copy(source, freqs, landing, which, j):
        start, count = freqs
        return pltpu.make_async_remote_copy(
            src_ref=source(j).at[pl.ds(start, count)], dst_ref=landing.at[pl.ds(FL * me_f + start, count)],
            send_sem=win_send.at[which, j], recv_sem=win_recv.at[which, me_f],
            device_id=(j, me_r), device_id_type=MESH)

    def in_wait(landing, freqs, which, sender):
        start, count = freqs
        where = landing.at[pl.ds(FL * sender + start, count)]
        pltpu.make_async_remote_copy(
            src_ref=where, dst_ref=where,
            send_sem=win_send.at[which, 0], recv_sem=win_recv.at[which, sender],
            device_id=(sender, me_r), device_id_type=MESH).wait_recv()

    def return_copy(clipped, target, which, d):
        return pltpu.make_async_remote_copy(
            src_ref=clipped.at[pl.ds(FL * d, FL)], dst_ref=target(me_f),
            send_sem=ret_send.at[which, d], recv_sem=ret_recv.at[which, me_f],
            device_id=(d, me_r), device_id_type=MESH)

    def return_wait(target, which, j):
        pltpu.make_async_remote_copy(
            src_ref=target(j), dst_ref=target(j), send_sem=ret_send.at[which, 0],
            recv_sem=ret_recv.at[which, j], device_id=(j, me_r), device_id_type=MESH).wait_recv()

    def window(landing, clipped, starts):
        half = lax.broadcasted_iota(jnp.int32, (NF * FL, 128), 1) < 64
        tops, bottoms = [], []
        for m in range(4):
            first, second = landing[:, 2 * m, :], landing[:, 2 * m + 1, :]
            tops.append(jnp.where(half, first, pltpu.roll(second, 64, 1)))
            bottoms.append(jnp.where(half, pltpu.roll(first, 64, 1), second))
        spectrum = jnp.concatenate([jnp.concatenate(tops, axis=1), jnp.concatenate(bottoms, axis=1)], axis=0)
        high, low = split(spectrum)
        traces = jnp.dot(inv[...], jnp.concatenate([high, low, high], axis=0), preferred_element_type=F32)
        limit = starts()
        limits = jnp.concatenate([limit[m : m + 1, :] for m in range(8)], axis=1)
        sample = lax.broadcasted_iota(jnp.int32, traces.shape, 0)
        kept = jnp.where(sample < limits, traces, 0.0)
        high, low = split(kept)
        again = jnp.dot(fwd[...], jnp.concatenate([high, low, high], axis=0), preferred_element_type=F32)
        for m in range(4):
            real = again[: NF * FL, 128 * m : 128 * m + 128]
            imag = again[NF * FL :, 128 * m : 128 * m + 128]
            clipped[:, 2 * m, :] = jnp.where(half, real, pltpu.roll(imag, 64, 1))
            clipped[:, 2 * m + 1, :] = jnp.where(half, pltpu.roll(real, 64, 1), imag)

    def window_tasks(which, tag, members, source, sends, landing, clipped, starts, target, rank):
        inside = (me_f >= members[0]) & (me_f <= members[-1])

        def scatter(freqs, row):
            def run():
                for j in members:
                    @pl.when(me_f != j)
                    def _():
                        out_copy(source, freqs, landing, row, j).start()

                    @pl.when(me_f == j)
                    def _():
                        start, count = freqs
                        landing[FL * j + start : FL * j + start + count] = source(j)[start : start + count]

            return run

        def apply():
            @pl.when(inside)
            def _():
                for sender in range(NF):
                    @pl.when(me_f != sender)
                    def _():
                        for freqs, row, _deps in sends:
                            in_wait(landing, freqs, row, sender)

                window(landing, clipped, starts)
                for d in range(NF):
                    @pl.when(me_f != d)
                    def _():
                        return_copy(clipped, target, which, d).start()

                target(me_f)[...] = clipped[pl.ds(FL * me_f, FL)]

        def collect():
            if which == 1:
                drain()
            for j in members:
                @pl.when(me_f != j)
                def _():
                    return_wait(target, which, j)

        def drain():
            for j in members:
                @pl.when(me_f != j)
                def _():
                    for freqs, row, _deps in sends:
                        out_copy(source, freqs, landing, row, j).wait_send()

            @pl.when(inside)
            def _():
                for d in range(NF):
                    @pl.when(me_f != d)
                    def _():
                        return_copy(clipped, target, which, d).wait_send()

        if which == 0:
            plan.add(tag + "drain", (tag + "in",) + ("w1in",), drain, dur=0.3, rank=(5,))
        outs = []
        for freqs, row, deps in sends:
            outs.append(f"{tag}out{row}")
            plan.add(outs[-1], deps, scatter(freqs, row), ("x", 0), len(members) * 8 * freqs[1] * 340, 0.2, rank)
        plan.add(tag + "win", outs, apply, ("x", 1), len(members) * 8 * FL * 340, 1.5, rank)
        plan.add(tag + "in", (tag + "win",), collect, dur=0.2, rank=rank)

    def onset_here():
        return onset[pl.ds(pl.multiple_of(8 * jnp.minimum(me_f, ROWS // 8 - 1), 8), 8), :]

    plan.add("onset", ("own0",), onset_ready, dur=0.05, rank=(0, 0, 0))
    for h in range(CHUNKS):
        def onset_summed(h=h):
            j = jnp.clip(me_f - MEMBERS * h, 0, MEMBERS - 1)
            return onset_own[h, pl.ds(pl.multiple_of(8 * j, 8), 8), :]

        members = tuple(range(MEMBERS * h, MEMBERS * h + MEMBERS))
        window_tasks(0, f"w{h}", members, functools.partial(block_of, part, h),
                     [((0, FL), 0, (f"own{h}", "onset"))], x1, y1, onset_summed,
                     functools.partial(block_of, gathered, h), (0, h, 0))

    def gather_piece(name, freqs, dz, dy, h, target, deps, link, rank):
        start, count = freqs
        where = gathered.at[pl.ds(start, count), h, at_z(dz), at_y(dy)]
        copy = piece(name, where, where, target, 1, h)
        arrivals = [dep for dep in deps if dep in copies]

        def run():
            for dep in arrivals:
                receive(dep)
            copy.start()

        plan.add(name, deps, run, link, count * NR * 512, 0.08, rank)

    received = set()

    def receive(name):
        if name not in received:
            received.add(name)
            copies[name].wait_recv()

    ends = {(h, name): [] for h in range(CHUNKS) for name in PARTS}
    for h in range(CHUNKS):
        own = f"w{h}in"
        deep = NZ // 2
        for sign in (1, -1):
            gather_piece(f"ya{h},{sign},0", PARTS["a"], 0, 0, h, rec_of(0, sign), (own,), ("y", sign), (2, h, 0))
            gather_piece(f"zb{h},{sign},0", PARTS["b"], 0, 0, h, rec_of(sign, 0), (own,), ("z", sign), (2, h, 0))
        for sign in (1, -1):
            gather_piece(f"ya{h},{sign},1", halves("a", sign), 0, -sign, h, rec_of(0, sign), (f"ya{h},{sign},0",),
                         ("y", sign), (2, h, 0))
            for k in range(1, deep):
                freqs = halves("b", sign) if k == deep - 1 else PARTS["b"]
                gather_piece(f"zb{h},{sign},{k}", freqs, -sign * k, 0, h, rec_of(sign, 0), (f"zb{h},{sign},{k - 1}",),
                             ("z", sign), (2, h, 0))
        for dy in (0, -1, 1, 2):
            if dy == 0:
                deps = (own,)
            elif dy == 2:
                deps = (f"ya{h},1,1", f"ya{h},-1,1")
            else:
                deps = (f"ya{h},{-dy},0",)
            for sign in (1, -1):
                for k in range(deep):
                    if k == deep - 1 and dy not in both_y[sign]:
                        continue
                    gather_piece(f"za{h},{sign},{k},{dy}", PARTS["a"], -sign * k, dy, h, rec_of(sign, 0),
                                 deps if k == 0 else (f"za{h},{sign},{k - 1},{dy}",), ("z", sign), (2, h, 1, k))
                    ends[h, "a"].append(f"za{h},{sign},{k},{dy}")
        for dz in (0, -1, 1, -2, 2, -3, 3, 4):
            if dz == 0:
                deps = (own,)
            elif dz == 4:
                deps = (f"zb{h},1,{deep - 1}", f"zb{h},-1,{deep - 1}")
            else:
                sign = -1 if dz > 0 else 1
                deps = (f"zb{h},{sign},{abs(dz) - 1}",)
            for sign in (1, -1):
                for k in range(2):
                    if k == 1 and dz not in both_z[sign]:
                        continue
                    gather_piece(f"yb{h},{sign},{k},{dz}", PARTS["b"], dz, -sign * k, h, rec_of(0, sign),
                                 deps if k == 0 else (f"yb{h},{sign},0,{dz}",), ("y", sign), (2, h, 1, k))
                    ends[h, "b"].append(f"yb{h},{sign},{k},{dz}")
        for name in list(copies):
            if name.startswith((f"ya{h}", f"zb{h}")):
                ends[h, name[1]].append(name)

    def forward(freqs, h, name):
        def run():
            for key in ends[h, name]:
                receive(key)

            def step(f, _):
                high, low = split(resp[f, :, pl.ds(COLS * h, COLS)])
                w_high, w_low = split(gathered[f, h].reshape(COLS, 128))
                terms = jnp.dot(jnp.concatenate([high, low], axis=0), jnp.concatenate([w_high, w_low], axis=1),
                                preferred_element_type=F32)
                total = terms[: 2 * ROWS, :128] + terms[: 2 * ROWS, 128:] + terms[2 * ROWS :, :128]
                if h > 0:
                    total = total + acc[f]
                if h < CHUNKS - 1:
                    acc[f] = total
                else:
                    turned = pltpu.roll(total[ROWS:], 64, 1)
                    made[f] = total[:ROWS] + jnp.where(low_half, -turned, turned)
                return _

            for f in freqs:
                step(f, 0)

        return run

    last = {}
    for h in range(CHUNKS):
        for name in PARTS:
            last[name] = []
            for place, freqs in enumerate(groups(name, 3 if h < CHUNKS - 1 else FL)):
                key = f"fwd{name}{h},{place}"
                last[name].append(key)
                before = [f"fwd{name}{h - 1},{p}" for p in range(len(groups(name, 3)))] if h else []
                plan.add(key, ends[h, name] + [f"w{h}in"] + before, forward(freqs, h, name),
                         dur=3.4 / CHUNKS * len(freqs) / FL, rank=(3, h))

    window_tasks(1, "v", tuple(range(ROWS // 8)), lambda j: made.at[:, pl.ds(8 * j, 8), :],
                 [(PARTS[name], 1 + place, last[name]) for place, name in enumerate(("b", "a"))], x2, y2, onset_here,
                 lambda j: back.at[:, pl.ds(8 * j, 8), :], (4,))

    order = plan.order()
    entered = False
    for _now, name in order:
        if plan.tasks[name][2] and not entered:
            enter()
            entered = True
        plan.tasks[name][1]()
    blocks = CHUNKS * FL * (NZ * NY - 1)
    for phase, buffer in enumerate((part, gathered)):
        amount = buffer.reshape(CHUNKS * FL * NZ * NY, NR, 128).at[pl.ds(0, blocks)]
        pltpu.make_async_copy(amount, amount, send_sem.at[phase]).wait()
    out[...] = back[...]
    kernel.plan = plan
    kernel.ordered = order


def iterate(response_real, response_imaginary, focus, onset, inv, fwd):
    na, nb = SPLIT, FL - SPLIT
    vmem = pl.BlockSpec(memory_space=pltpu.VMEM)
    scratch = [
        pltpu.VMEM(focus.shape, F32),
        pltpu.VMEM(onset.shape, jnp.int32),
        pltpu.VMEM(inv.shape, BF),
        pltpu.VMEM(fwd.shape, BF),
        pltpu.SemaphoreType.DMA((4,)),
        pltpu.VMEM((FL, 2 * ROWS, response_real.shape[2]), F32),
        pltpu.SemaphoreType.DMA((2, CHUNKS, 2)),
        pltpu.VMEM((FL, CHUNKS, NZ, NY, NR, 128), F32),
        pltpu.VMEM((28 * CHUNKS, na, NR, 128), F32),
        pltpu.VMEM((4 * CHUNKS, na, NR, 128), F32),
        pltpu.VMEM((24 * CHUNKS, nb, NR, 128), F32),
        pltpu.VMEM((8 * CHUNKS, nb, NR, 128), F32),
        pltpu.VMEM((FL, CHUNKS, NZ, NY, NR, 128), F32),
        pltpu.VMEM((FL, 2 * ROWS, 128), F32),
        pltpu.VMEM((NF * FL, 8, 128), F32),
        pltpu.VMEM((NF * FL, 8, 128), F32),
        pltpu.VMEM((NF * FL, 8, 128), F32),
        pltpu.VMEM((NF * FL, 8, 128), F32),
        pltpu.VMEM((FL, 2 * ROWS, 128), F32),
        pltpu.VMEM((FL, ROWS, 128), F32),
        pltpu.VMEM((FL, ROWS, 128), F32),
        pltpu.VMEM((CHUNKS, NR, onset.shape[1]), jnp.int32),
        pltpu.SemaphoreType.DMA((CHUNKS,)),
        pltpu.SemaphoreType.DMA((CHUNKS,)),
        pltpu.SemaphoreType.DMA((2,)),
        pltpu.SemaphoreType.DMA((2 * CHUNKS - 1, 64)),
        pltpu.SemaphoreType.DMA((3, NF)),
        pltpu.SemaphoreType.DMA((3, NF)),
        pltpu.SemaphoreType.DMA((2, NF)),
        pltpu.SemaphoreType.DMA((2, NF)),
    ]
    return pl.pallas_call(
        kernel,
        out_shape=jax.ShapeDtypeStruct((FL, ROWS, 128), F32),
        in_specs=[pl.BlockSpec(memory_space=pl.ANY)] * 6,
        out_specs=vmem,
        scratch_shapes=scratch,
        compiler_params=pltpu.CompilerParams(
            collective_id=0, has_side_effects=True, vmem_limit_bytes=60 * 1024 * 1024
        ),
    )(response_real, response_imaginary, focus, onset, inv, fwd)


def on_device(response_real, response_imaginary, focus, initial, onset):
    inv, fwd = dft_tables(NF * FL)
    by_freq = jnp.transpose(focus, (1, 0, 2))
    update = iterate(response_real, response_imaginary, by_freq, onset, jnp.asarray(inv), jnp.asarray(fwd))
    return initial - jnp.transpose(update, (1, 0, 2))


def solution(mesh):
    in_specs = (
        P("freq", "rec", None),
        P("freq", "rec", None),
        P("rec", "freq", None),
        P("rec", "freq", None),
        P("rec", None),
    )
    return jax.shard_map(
        on_device, mesh=mesh, in_specs=in_specs, out_specs=P("rec", "freq", None), check_vma=False
    )
```

```python
import functools
import heapq

import jax
import jax.numpy as jnp
import numpy as np
from jax import lax
from jax.experimental import pallas as pl
from jax.experimental.pallas import tpu as pltpu
from jax.sharding import PartitionSpec as P

MESH = pl.DeviceIdType.MESH
BF = jnp.bfloat16
F32 = jnp.float32

NF = 8
NZ, NY = 8, 4
FL = 12
ROWS = 48
SPLIT = 5
CHUNKS = 2
NR = ROWS // CHUNKS
COLS = NZ * NY * NR
MEMBERS = NR // 8
RATE = 46.6e3
LATENCY = 1.8
ADJ, FWD = 0, 0
X_LATENCY = 4.0
BACKLOG = 1.0


def split(value):
    high = value.astype(BF)
    low = (value - high.astype(F32)).astype(BF)
    return high, low


def dft_tables(freqs):
    samples = 2 * freqs
    phase = np.arange(freqs)[:, None] * np.arange(samples)[None, :] % samples
    angle = 2.0 * np.pi / samples * phase
    cosine, sine = np.cos(angle), np.sin(angle)
    factor = np.where(np.arange(freqs) == 0, 1.0, 2.0)[:, None] / samples
    inverse = np.concatenate([factor * cosine, -factor * sine]).T
    forward = np.concatenate([cosine, -sine])
    out = []
    for table in (inverse, forward):
        table = table.astype(np.float32)
        high = table.astype(jnp.bfloat16)
        low = (table - high.astype(np.float32)).astype(jnp.bfloat16)
        out.append(np.concatenate([high, high, low], axis=1))
    return out


PARTS = {"a": (0, SPLIT), "b": (SPLIT, FL - SPLIT)}


def halves(part, sign):
    start, count = PARTS[part]
    first = (count + 1) // 2 if part == "a" else count // 2
    return (start, first) if sign > 0 else (start + first, count - first)


class Plan:
    def __init__(self):
        self.tasks, self.sent = {}, {}

    def add(self, name, deps, run, link=None, size=0, dur=0.1, rank=(0,)):
        self.tasks[name] = (tuple(deps), run, link, size, dur, rank)

    def order(self):
        free, arrived, done = {}, {}, {}
        left = dict(self.tasks)
        now, order = 0.0, []
        while left:
            ready, soonest = [], None
            for name, (deps, run, link, size, dur, rank) in left.items():
                when = 0.0
                for dep in deps:
                    when = max(when, arrived.get(dep, 1e9))
                if link is not None:
                    when = max(when, free.get(link, 0.0) - BACKLOG)
                if when <= now:
                    ready.append((rank, name))
                soonest = when if soonest is None else min(soonest, when)
            if not ready:
                if soonest >= 1e9:
                    raise ValueError("cycle")
                now = soonest
                continue
            _, name = min(ready)
            deps, run, link, size, dur, rank = left.pop(name)
            now += dur
            order.append((now, name))
            if link is None:
                arrived[name] = now
            else:
                start = max(now, free.get(link, 0.0))
                free[link] = start + size / RATE
                arrived[name] = free[link] + (LATENCY if link[0] != "x" else X_LATENCY)
                self.sent[name] = free[link]
            done[name] = now
        self.finish = now
        self.times = arrived
        return order


def kernel(rr, ri, focus_in, onset_in, inv_in, fwd_in, initial_in, out, *scratch):
    (focus, onset, inv, fwd, initial, small_sem, resp, load_sem, part, stage_a1, stage_a2, stage_b1, stage_b2, gathered, xs, x1, y1, x2, y2, acc, made, back,
     onset_own, onset_send, onset_recv, send_sem, recv_sem, win_send, win_recv, ret_send, ret_recv) = scratch
    me_f, me_r = lax.axis_index("freq"), lax.axis_index("rec")
    z, y = lax.div(me_r, NY), lax.rem(me_r, NY)

    def at_z(d):
        return lax.rem(z + (d + NZ), NZ) if d else z

    def at_y(d):
        return lax.rem(y + (d + NY), NY) if d else y

    def rec_of(dz, dy):
        return at_z(dz) * NY + at_y(dy)

    def load(c, h, name):
        start, count = PARTS[name]
        cols, freqs = pl.ds(COLS * h, COLS), pl.ds(start, count)
        return pltpu.make_async_copy(
            (rr, ri)[c].at[freqs, :, cols], resp.at[freqs, pl.ds(ROWS * c, ROWS), cols],
            load_sem.at[c, h, list(PARTS).index(name)])

    small = [pltpu.make_async_copy(src, dst, small_sem.at[i]) for i, (src, dst) in enumerate(
        ((focus_in, focus), (onset_in, onset), (inv_in, inv), (fwd_in, fwd), (initial_in, initial)))]
    small[0].start()
    for h in range(CHUNKS):
        for name in PARTS:
            load(0, h, name).start()
            load(1, h, name).start()
        if h == 0:
            for copy in small[1:]:
                copy.start()

    barrier = pltpu.get_barrier_semaphore()
    for dz, dy in ((1, 0), (-1, 0), (0, 1), (0, -1)):
        pl.semaphore_signal(barrier, inc=1, device_id=(me_f, rec_of(dz, dy)), device_id_type=MESH)
    for d in range(1, NF):
        pl.semaphore_signal(barrier, inc=1, device_id=(lax.rem(me_f + d, NF), me_r), device_id_type=MESH)

    def onset_source(h):
        return lax.div(h * NZ * NY + me_r, CHUNKS)

    def onset_copy(u):
        index = me_r * CHUNKS + u
        target, h = lax.rem(index, NZ * NY), lax.div(index, NZ * NY)
        rows = onset.at[pl.ds(NR * u, NR), :]
        return target, h, rows, pltpu.make_async_remote_copy(
            src_ref=rows, dst_ref=onset_own.at[h], send_sem=onset_send.at[u], recv_sem=onset_recv.at[h],
            device_id=(me_f, target), device_id_type=MESH)

    for h in range(CHUNKS):
        @pl.when(onset_source(h) != me_r)
        def _():
            pl.semaphore_signal(barrier, inc=1, device_id=(me_f, onset_source(h)), device_id_type=MESH)

    def enter():
        for copy in small[1:]:
            copy.wait()
        peers = 4 + NF - 1
        for u in range(CHUNKS):
            peers += jnp.where(lax.rem(me_r * CHUNKS + u, NZ * NY) != me_r, 1, 0)
        pl.semaphore_wait(barrier, peers)
        for u in range(CHUNKS):
            target, h, rows, copy = onset_copy(u)

            @pl.when(target != me_r)
            def _():
                copy.start()

            @pl.when(target == me_r)
            def _():
                onset_own[h] = rows[...]

    def onset_ready():
        for u in range(CHUNKS):
            target, _h, _rows, copy = onset_copy(u)

            @pl.when(target != me_r)
            def _():
                copy.wait_send()

        for h in range(CHUNKS):
            @pl.when(onset_source(h) != me_r)
            def _():
                pltpu.make_async_remote_copy(
                    src_ref=onset_own.at[h], dst_ref=onset_own.at[h], send_sem=onset_send.at[0],
                    recv_sem=onset_recv.at[h], device_id=(me_f, me_r), device_id_type=MESH).wait_recv()

    lane = lax.broadcasted_iota(jnp.int32, (ROWS, 128), 1)
    low_half = lane < 64
    plan = Plan()
    copies = {}

    used = {}

    def piece(name, src, dst, target, phase, h):
        bank = h if phase == 0 else (CHUNKS + h if h < CHUNKS - 1 else 0)
        index = used[phase, h] = used.get((phase, h), -1) + 1
        copies[name] = pltpu.make_async_remote_copy(
            src_ref=src, dst_ref=dst, send_sem=send_sem.at[phase], recv_sem=recv_sem.at[bank, index],
            device_id=(me_f, target), device_id_type=MESH)
        return copies[name]

    def each(freqs, step, together):
        whole = len(freqs) // together * together if together else 0
        if whole > together:
            def body(i, carry):
                for k in range(together):
                    step(freqs[0] + i * together + k, 0)
                return carry

            lax.fori_loop(0, whole // together, body, 0)
        else:
            whole = 0
        for f in freqs[whole:]:
            step(f, 0)

    small[0].wait()
    for f in range(FL):
        value = focus[f]
        turned = pltpu.roll(value, 64, 1)
        xs[f, 0:ROWS, :] = value
        xs[f, ROWS : 2 * ROWS, :] = jnp.where(low_half, turned, -turned)

    def adjoint(freqs, h, name):
        def run():
            if freqs[0] == PARTS[name][0]:
                load(0, h, name).wait()
                load(1, h, name).wait()

            def step(f, _):
                x_high, x_low = split(xs[f])
                left = jnp.concatenate([x_high, x_high], axis=0)
                right = jnp.concatenate([x_low, jnp.zeros_like(x_low)], axis=0)
                both = jnp.concatenate([left, right], axis=1)
                for c in range(2):
                    high, low = split(resp[f, :, pl.ds(COLS * h + COLS // 2 * c, COLS // 2)])
                    terms = lax.dot_general(jnp.concatenate([high, low], axis=0), both, (((0,), (0,)), ((), ())),
                                            preferred_element_type=F32)
                    total = terms[:, :128] + terms[:, 128:]
                    part[f, h, NZ // 2 * c : NZ // 2 * (c + 1)] = total.reshape(NZ // 2, NY, NR, 128)
                return _

            each(freqs, step, ADJ)

        return run

    def groups(name, size):
        start, count = PARTS[name]
        return [tuple(range(f, min(f + size, start + count))) for f in range(start, start + count, size)]

    adjoint_done = {}
    for h in range(CHUNKS):
        for name in ("a", "b"):
            adjoint_done[h, name] = []
            for place, freqs in enumerate(groups(name, FL if h == 0 else 3)):
                key = f"adj{name}{h},{place}"
                adjoint_done[h, name].append(key)
                plan.add(key, (), adjoint(freqs, h, name), dur=3.4 / CHUNKS * len(freqs) / FL, rank=(0 if h == 0 else 1, max(h - 1, 0), 9, name != "a", place))

    slot = {"a1": 0, "a2": 0, "b1": 0, "b2": 0}
    stages = {"a1": stage_a1, "a2": stage_a2, "b1": stage_b1, "b2": stage_b2}

    def staging(kind, count):
        index = slot[kind]
        slot[kind] += 1
        return stages[kind].at[index, pl.ds(0, count)]

    def reduce_piece(name, kind, freqs, dz, dy, h, target, adds, deps, link, rank):
        start, count = freqs
        src = part.at[pl.ds(start, count), h, at_z(dz), at_y(dy)]
        dst = staging(kind, count)
        copy = piece(name, src, dst, target, 0, h)
        copies[name] = (copy, dst, start, count)

        def run():
            take(adds, dz, dy, h)
            copy.start()

        plan.add(name, tuple(adds) + tuple(deps), run, link, count * NR * 512, 0.12, rank)

    def take(adds, dz, dy, h):
        for other in adds:
            copy, dst, start, count = copies[other]
            copy.wait_recv()
            where = (pl.ds(start, count), h, at_z(dz), at_y(dy))
            part[where] += dst[...]

    for h in range(CHUNKS):
        deep = NZ // 2
        order_y = (2, 1, -1, 0)
        order_z = (4, 3, -3, 2, -2, 1, -1, 0)
        both_y = {1: (2, 0), -1: (1, -1)}
        both_z = {1: (4, 2, -2, 0), -1: (3, -3, 1, -1)}
        for k in range(deep, 0, -1):
            for place, dy in enumerate(order_y):
                for sign in (1, -1):
                    if k == deep and dy not in both_y[sign]:
                        continue
                    adds = [f"a1{h},{sign},{k + 1},{dy}"] if (k < deep - 1 or (k == deep - 1 and dy in both_y[sign])) else []
                    reduce_piece(f"a1{h},{sign},{k},{dy}", "a1", PARTS["a"], sign * k, dy, h, rec_of(sign, 0), adds,
                                 adjoint_done[h, "a"], ("z", sign), (1, h, 0, -k, place))
        for k in (2, 1):
            for place, dz in enumerate(order_z):
                for sign in (1, -1):
                    if k == 2 and dz not in both_z[sign]:
                        continue
                    adds = [f"b1{h},{sign},2,{dz}"] if k == 1 and dz in both_z[sign] else []
                    reduce_piece(f"b1{h},{sign},{k},{dz}", "b1", PARTS["b"], dz, sign * k, h, rec_of(0, sign), adds,
                                 adjoint_done[h, "b"], ("y", sign), (1, h, 0, -k, place))

        def first_sum(name, kind, d):
            keys = [f"{kind}{h},{sign},1,{d}" for sign in (1, -1)]

            def run(keys=keys, d=d, h=h, kind=kind):
                dz, dy = (0, d) if kind == "a1" else (d, 0)
                take(keys, dz, dy, h)

            plan.add(name, keys, run, dur=0.12, rank=(0, h, 0))

        for dy in order_y:
            first_sum(f"as{h},{dy}", "a1", dy)
        for dz in order_z:
            first_sum(f"bs{h},{dz}", "b1", dz)
        for sign in (1, -1):
            reduce_piece(f"a2{h},{sign},2", "a2", halves("a", sign), 0, 2 * sign, h, rec_of(0, sign), [],
                         (f"as{h},2",), ("y", sign), (0, h, 1, -2))
            reduce_piece(f"a2{h},{sign},1", "a2", PARTS["a"], 0, sign, h, rec_of(0, sign), [f"a2{h},{sign},2"],
                         (f"as{h},{sign}",), ("y", sign), (0, h, 1, -1))
            for k in range(deep, 0, -1):
                freqs = halves("b", sign) if k == deep else PARTS["b"]
                adds = [] if k == deep else [f"b2{h},{sign},{k + 1}"]
                source = 4 if k == deep else sign * k
                reduce_piece(f"b2{h},{sign},{k}", "b2", freqs, sign * k, 0, h, rec_of(sign, 0), adds,
                             (f"bs{h},{source}",), ("z", sign), (0, h, 1, -k))

        own_keys = [f"a2{h},{sign},1" for sign in (1, -1)] + [f"b2{h},{sign},1" for sign in (1, -1)]

        def own_sum(keys=tuple(own_keys), h=h):
            take(keys, 0, 0, h)

        plan.add(f"own{h}", own_keys + [f"as{h},0", f"bs{h},0"], own_sum, dur=0.2, rank=(0, h, 0))

    def block_of(buffer, h, j):
        return buffer.at[:, h, z, y, pl.ds(8 * (j - MEMBERS * h), 8), :]

    def out_copy(source, freqs, landing, row, j):
        start, count = freqs
        return pltpu.make_async_remote_copy(
            src_ref=source(j).at[pl.ds(start, count)], dst_ref=landing.at[pl.ds(FL * me_f + start, count)],
            send_sem=win_send.at[row], recv_sem=win_recv.at[row], device_id=(j, me_r), device_id_type=MESH)

    def return_copy(clipped, target, row, d):
        return pltpu.make_async_remote_copy(
            src_ref=clipped.at[pl.ds(FL * d, FL)], dst_ref=target(me_f),
            send_sem=ret_send.at[row], recv_sem=ret_recv.at[row], device_id=(d, me_r), device_id_type=MESH)

    def wait_tiles(buffer, count, sem):
        tiles = buffer.at[pl.ds(0, count)]
        pltpu.make_async_copy(tiles, tiles, sem).wait()

    def window(landing, clipped, starts):
        half = lax.broadcasted_iota(jnp.int32, (NF * FL, 128), 1) < 64
        tops, bottoms = [], []
        for m in range(4):
            first, second = landing[:, 2 * m, :], landing[:, 2 * m + 1, :]
            tops.append(jnp.where(half, first, pltpu.roll(second, 64, 1)))
            bottoms.append(jnp.where(half, pltpu.roll(first, 64, 1), second))
        spectrum = jnp.concatenate([jnp.concatenate(tops, axis=1), jnp.concatenate(bottoms, axis=1)], axis=0)
        high, low = split(spectrum)
        traces = jnp.dot(inv[...], jnp.concatenate([high, low, high], axis=0), preferred_element_type=F32)
        limit = starts()
        limits = jnp.concatenate([limit[m : m + 1, :] for m in range(8)], axis=1)
        sample = lax.broadcasted_iota(jnp.int32, traces.shape, 0)
        kept = jnp.where(sample < limits, traces, 0.0)
        high, low = split(kept)
        again = jnp.dot(fwd[...], jnp.concatenate([high, low, high], axis=0), preferred_element_type=F32)
        for m in range(4):
            real = again[: NF * FL, 128 * m : 128 * m + 128]
            imag = again[NF * FL :, 128 * m : 128 * m + 128]
            clipped[:, 2 * m, :] = jnp.where(half, real, pltpu.roll(imag, 64, 1))
            clipped[:, 2 * m + 1, :] = jnp.where(half, pltpu.roll(real, 64, 1), imag)

    def window_tasks(which, tag, members, source, sends, landing, clipped, starts, target, rank):
        inside = (me_f >= members[0]) & (me_f <= members[-1])
        returns = sends[0][1]

        def others(run):
            @pl.when(inside)
            def _():
                run(len(members) - 1)

            @pl.when(jnp.logical_not(inside))
            def _():
                run(len(members))

        def scatter(freqs, row):
            def run():
                for j in members:
                    @pl.when(me_f != j)
                    def _():
                        out_copy(source, freqs, landing, row, j).start()

                    @pl.when(me_f == j)
                    def _():
                        start, count = freqs
                        landing[FL * j + start : FL * j + start + count] = source(j)[start : start + count]

            return run

        def apply():
            @pl.when(inside)
            def _():
                for freqs, row, _deps in sends:
                    wait_tiles(landing, (NF - 1) * freqs[1], win_recv.at[row])
                window(landing, clipped, starts)
                for d in range(NF):
                    @pl.when(me_f != d)
                    def _():
                        return_copy(clipped, target, returns, d).start()

                target(me_f)[...] = clipped[pl.ds(FL * me_f, FL)]

        def drain():
            for freqs, row, _deps in sends:
                others(lambda n: wait_tiles(landing, n * freqs[1], win_send.at[row]))

            @pl.when(inside)
            def _():
                wait_tiles(landing, (NF - 1) * FL, ret_send.at[returns])

        def collect():
            others(lambda n: wait_tiles(landing, n * FL, ret_recv.at[returns]))
            if which == 1:
                drain()

        if which == 0:
            plan.add(tag + "drain", (tag + "in",) + ("w1in",), drain, dur=0.3, rank=(5,))
        outs = []
        for freqs, row, deps in sends:
            outs.append(f"{tag}out{row}")
            plan.add(outs[-1], deps, scatter(freqs, row), ("x", 0), len(members) * 8 * freqs[1] * 340, 0.2, rank if which == 0 else (2, 9))
        plan.add(tag + "win", outs, apply, ("x", 1), len(members) * 8 * FL * 340, 1.5, rank)
        plan.add(tag + "in", (tag + "win",), collect, dur=0.2, rank=rank)

    def onset_here():
        return onset[pl.ds(pl.multiple_of(8 * jnp.minimum(me_f, ROWS // 8 - 1), 8), 8), :]

    plan.add("onset", ("own0",), onset_ready, dur=0.05, rank=(0, 0, 0))
    for h in range(CHUNKS):
        def onset_summed(h=h):
            j = jnp.clip(me_f - MEMBERS * h, 0, MEMBERS - 1)
            return onset_own[h, pl.ds(pl.multiple_of(8 * j, 8), 8), :]

        members = tuple(range(MEMBERS * h, MEMBERS * h + MEMBERS))
        window_tasks(0, f"w{h}", members, functools.partial(block_of, part, h),
                     [((0, FL), h, (f"own{h}", "onset"))], x1, y1, onset_summed,
                     functools.partial(block_of, gathered, h), (0, h, 0))

    def gather_piece(name, freqs, dz, dy, h, target, deps, link, rank):
        start, count = freqs
        where = gathered.at[pl.ds(start, count), h, at_z(dz), at_y(dy)]
        copy = piece(name, where, where, target, 1, h)
        arrivals = [dep for dep in deps if dep in copies]

        def run():
            for dep in arrivals:
                receive(dep)
            copy.start()

        plan.add(name, deps, run, link, count * NR * 512, 0.08, rank)

    received = set()

    def receive(name):
        if name not in received:
            received.add(name)
            copies[name].wait_recv()

    ends = {(h, name): [] for h in range(CHUNKS) for name in PARTS}
    for h in range(CHUNKS):
        own = f"w{h}in"
        deep = NZ // 2
        for sign in (1, -1):
            gather_piece(f"ya{h},{sign},0", PARTS["a"], 0, 0, h, rec_of(0, sign), (own,), ("y", sign), (2, 0, h))
            gather_piece(f"zb{h},{sign},0", PARTS["b"], 0, 0, h, rec_of(sign, 0), (own,), ("z", sign), (2, 0, h))
        for sign in (1, -1):
            gather_piece(f"ya{h},{sign},1", halves("a", sign), 0, -sign, h, rec_of(0, sign), (f"ya{h},{sign},0",),
                         ("y", sign), (2, 0, h))
            for k in range(1, deep):
                freqs = halves("b", sign) if k == deep - 1 else PARTS["b"]
                gather_piece(f"zb{h},{sign},{k}", freqs, -sign * k, 0, h, rec_of(sign, 0), (f"zb{h},{sign},{k - 1}",),
                             ("z", sign), (2, 0, h))
        for dy in (0, -1, 1, 2):
            if dy == 0:
                deps = (own,)
            elif dy == 2:
                deps = (f"ya{h},1,1", f"ya{h},-1,1")
            else:
                deps = (f"ya{h},{-dy},0",)
            for sign in (1, -1):
                for k in range(deep):
                    if k == deep - 1 and dy not in both_y[sign]:
                        continue
                    gather_piece(f"za{h},{sign},{k},{dy}", PARTS["a"], -sign * k, dy, h, rec_of(sign, 0),
                                 deps if k == 0 else (f"za{h},{sign},{k - 1},{dy}",), ("z", sign), (2, 1, h, k))
                    ends[h, "a"].append(f"za{h},{sign},{k},{dy}")
        for dz in (0, -1, 1, -2, 2, -3, 3, 4):
            if dz == 0:
                deps = (own,)
            elif dz == 4:
                deps = (f"zb{h},1,{deep - 1}", f"zb{h},-1,{deep - 1}")
            else:
                sign = -1 if dz > 0 else 1
                deps = (f"zb{h},{sign},{abs(dz) - 1}",)
            for sign in (1, -1):
                for k in range(2):
                    if k == 1 and dz not in both_z[sign]:
                        continue
                    gather_piece(f"yb{h},{sign},{k},{dz}", PARTS["b"], dz, -sign * k, h, rec_of(0, sign),
                                 deps if k == 0 else (f"yb{h},{sign},0,{dz}",), ("y", sign), (2, 1, h, k))
                    ends[h, "b"].append(f"yb{h},{sign},{k},{dz}")
        for name in list(copies):
            if name.startswith((f"ya{h}", f"zb{h}")):
                ends[h, name[1]].append(name)

    def forward(freqs, h, name):
        def run():
            for key in ends[h, name]:
                receive(key)

            def step(f, _):
                high, low = split(resp[f, :, pl.ds(COLS * h, COLS)])
                w_high, w_low = split(gathered[f, h].reshape(COLS, 128))
                terms = jnp.dot(jnp.concatenate([high, low], axis=0), jnp.concatenate([w_high, w_low], axis=1),
                                preferred_element_type=F32)
                total = terms[: 2 * ROWS, :128] + terms[: 2 * ROWS, 128:] + terms[2 * ROWS :, :128]
                if h > 0:
                    total = total + acc[f]
                if h < CHUNKS - 1:
                    acc[f] = total
                else:
                    turned = pltpu.roll(total[ROWS:], 64, 1)
                    made[f] = total[:ROWS] + jnp.where(low_half, -turned, turned)
                return _

            each(freqs, step, FWD)

        return run

    last = {}
    for h in range(CHUNKS):
        for name in PARTS:
            last[name] = []
            for place, freqs in enumerate(groups(name, 3 if h < CHUNKS - 1 else FL)):
                key = f"fwd{name}{h},{place}"
                last[name].append(key)
                before = [f"fwd{name}{h - 1},{p}" for p in range(len(groups(name, 3)))] if h else []
                plan.add(key, ends[h, name] + [f"w{h}in"] + before, forward(freqs, h, name),
                         dur=3.4 / CHUNKS * len(freqs) / FL, rank=(3, h))

    window_tasks(1, "v", tuple(range(ROWS // 8)), lambda j: made.at[:, pl.ds(8 * j, 8), :],
                 [(PARTS[name], CHUNKS + place, last[name]) for place, name in enumerate(("b", "a"))], x2, y2, onset_here,
                 lambda j: back.at[:, pl.ds(8 * j, 8), :], (4,))

    order = plan.order()
    entered = False
    for _now, name in order:
        if plan.tasks[name][2] and not entered:
            enter()
            entered = True
        plan.tasks[name][1]()
    blocks = CHUNKS * FL * (NZ * NY - 1)
    for phase, buffer in enumerate((part, gathered)):
        amount = buffer.reshape(CHUNKS * FL * NZ * NY, NR, 128).at[pl.ds(0, blocks)]
        pltpu.make_async_copy(amount, amount, send_sem.at[phase]).wait()
    out[...] = initial[...] - back[...]
    kernel.plan = plan
    kernel.ordered = order


def iterate(response_real, response_imaginary, focus, onset, inv, fwd, initial):
    na, nb = SPLIT, FL - SPLIT
    vmem = pl.BlockSpec(memory_space=pltpu.VMEM)
    scratch = [
        pltpu.VMEM(focus.shape, F32),
        pltpu.VMEM(onset.shape, jnp.int32),
        pltpu.VMEM(inv.shape, BF),
        pltpu.VMEM(fwd.shape, BF),
        pltpu.VMEM(focus.shape, F32),
        pltpu.SemaphoreType.DMA((5,)),
        pltpu.VMEM((FL, 2 * ROWS, response_real.shape[2]), F32),
        pltpu.SemaphoreType.DMA((2, CHUNKS, 2)),
        pltpu.VMEM((FL, CHUNKS, NZ, NY, NR, 128), F32),
        pltpu.VMEM((28 * CHUNKS, na, NR, 128), F32),
        pltpu.VMEM((4 * CHUNKS, na, NR, 128), F32),
        pltpu.VMEM((24 * CHUNKS, nb, NR, 128), F32),
        pltpu.VMEM((8 * CHUNKS, nb, NR, 128), F32),
        pltpu.VMEM((FL, CHUNKS, NZ, NY, NR, 128), F32),
        pltpu.VMEM((FL, 2 * ROWS, 128), F32),
        pltpu.VMEM((NF * FL, 8, 128), F32),
        pltpu.VMEM((NF * FL, 8, 128), F32),
        pltpu.VMEM((NF * FL, 8, 128), F32),
        pltpu.VMEM((NF * FL, 8, 128), F32),
        pltpu.VMEM((FL, 2 * ROWS, 128), F32),
        pltpu.VMEM((FL, ROWS, 128), F32),
        pltpu.VMEM((FL, ROWS, 128), F32),
        pltpu.VMEM((CHUNKS, NR, onset.shape[1]), jnp.int32),
        pltpu.SemaphoreType.DMA((CHUNKS,)),
        pltpu.SemaphoreType.DMA((CHUNKS,)),
        pltpu.SemaphoreType.DMA((2,)),
        pltpu.SemaphoreType.DMA((2 * CHUNKS - 1, 64)),
        pltpu.SemaphoreType.DMA((CHUNKS + 2,)),
        pltpu.SemaphoreType.DMA((CHUNKS + 2,)),
        pltpu.SemaphoreType.DMA((CHUNKS + 1,)),
        pltpu.SemaphoreType.DMA((CHUNKS + 1,)),
    ]
    return pl.pallas_call(
        kernel,
        out_shape=jax.ShapeDtypeStruct((FL, ROWS, 128), F32),
        in_specs=[pl.BlockSpec(memory_space=pl.ANY)] * 7,
        out_specs=vmem,
        scratch_shapes=scratch,
        compiler_params=pltpu.CompilerParams(
            collective_id=0, has_side_effects=True, vmem_limit_bytes=60 * 1024 * 1024
        ),
    )(response_real, response_imaginary, focus, onset, inv, fwd, initial)


def on_device(response_real, response_imaginary, focus, initial, onset):
    inv, fwd = dft_tables(NF * FL)
    by_freq = jnp.transpose(focus, (1, 0, 2))
    update = iterate(response_real, response_imaginary, by_freq, onset, jnp.asarray(inv), jnp.asarray(fwd),
                     jnp.transpose(initial, (1, 0, 2)))
    return jnp.transpose(update, (1, 0, 2))


def solution(mesh):
    in_specs = (
        P("freq", "rec", None),
        P("freq", "rec", None),
        P("rec", "freq", None),
        P("rec", "freq", None),
        P("rec", None),
    )
    return jax.shard_map(
        on_device, mesh=mesh, in_specs=in_specs, out_specs=P("rec", "freq", None), check_vma=False
    )
```

```python
import functools
import heapq

import jax
import jax.numpy as jnp
import numpy as np
from jax import lax
from jax.experimental import pallas as pl
from jax.experimental.pallas import tpu as pltpu
from jax.sharding import PartitionSpec as P

MESH = pl.DeviceIdType.MESH
BF = jnp.bfloat16
F32 = jnp.float32

NF = 8
NZ, NY = 8, 4
FL = 12
ROWS = 48
SPLIT = 5
CHUNKS = 2
NR = ROWS // CHUNKS
COLS = NZ * NY * NR
MEMBERS = NR // 8
RATE = 46.6e3
LATENCY = 1.8
ADJ, FWD = 0, 0
X_LATENCY = 4.0
BACKLOG = 1.4


def split(value):
    high = value.astype(BF)
    low = (value - high.astype(F32)).astype(BF)
    return high, low


def dft_tables(freqs):
    samples = 2 * freqs
    phase = np.arange(freqs)[:, None] * np.arange(samples)[None, :] % samples
    angle = 2.0 * np.pi / samples * phase
    cosine, sine = np.cos(angle), np.sin(angle)
    factor = np.where(np.arange(freqs) == 0, 1.0, 2.0)[:, None] / samples
    inverse = np.concatenate([factor * cosine, -factor * sine]).T
    forward = np.concatenate([cosine, -sine])
    out = []
    for table in (inverse, forward):
        table = table.astype(np.float32)
        high = table.astype(jnp.bfloat16)
        low = (table - high.astype(np.float32)).astype(jnp.bfloat16)
        out.append(np.concatenate([high, high, low], axis=1))
    return out


PARTS = {"a": (0, SPLIT), "b": (SPLIT, FL - SPLIT)}


def halves(part, sign):
    start, count = PARTS[part]
    first = (count + 1) // 2 if part == "a" else count // 2
    return (start, first) if sign > 0 else (start + first, count - first)


class Plan:
    def __init__(self):
        self.tasks, self.sent = {}, {}

    def add(self, name, deps, run, link=None, size=0, dur=0.1, rank=(0,)):
        self.tasks[name] = (tuple(deps), run, link, size, dur, rank)

    def order(self):
        free, arrived, done = {}, {}, {}
        left = dict(self.tasks)
        now, order = 0.0, []
        while left:
            ready, soonest = [], None
            for name, (deps, run, link, size, dur, rank) in left.items():
                when = 0.0
                for dep in deps:
                    when = max(when, arrived.get(dep, 1e9))
                if link is not None:
                    when = max(when, free.get(link, 0.0) - BACKLOG)
                if when <= now:
                    ready.append((rank, name))
                soonest = when if soonest is None else min(soonest, when)
            if not ready:
                if soonest >= 1e9:
                    raise ValueError("cycle")
                now = soonest
                continue
            _, name = min(ready)
            deps, run, link, size, dur, rank = left.pop(name)
            now += dur
            order.append((now, name))
            if link is None:
                arrived[name] = now
            else:
                start = max(now, free.get(link, 0.0))
                free[link] = start + size / RATE
                arrived[name] = free[link] + (LATENCY if link[0] != "x" else X_LATENCY)
                self.sent[name] = free[link]
            done[name] = now
        self.finish = now
        self.times = arrived
        return order


def kernel(rr, ri, focus_in, onset_in, inv_in, fwd_in, initial_in, out, *scratch):
    (focus, onset, inv, fwd, initial, small_sem, resp, load_sem, part, stage_a1, stage_a2, stage_b1, stage_b2, gathered, xs, x1, y1, x2, y2, acc, made, back,
     onset_own, onset_send, onset_recv, send_sem, recv_sem, win_send, win_recv, ret_send, ret_recv) = scratch
    me_f, me_r = lax.axis_index("freq"), lax.axis_index("rec")
    z, y = lax.div(me_r, NY), lax.rem(me_r, NY)

    def at_z(d):
        return lax.rem(z + (d + NZ), NZ) if d else z

    def at_y(d):
        return lax.rem(y + (d + NY), NY) if d else y

    def rec_of(dz, dy):
        return at_z(dz) * NY + at_y(dy)

    def load(c, h, name):
        start, count = PARTS[name]
        cols, freqs = pl.ds(COLS * h, COLS), pl.ds(start, count)
        return pltpu.make_async_copy(
            (rr, ri)[c].at[freqs, :, cols], resp.at[freqs, pl.ds(ROWS * c, ROWS), cols],
            load_sem.at[c, h, list(PARTS).index(name)])

    small = [pltpu.make_async_copy(src, dst, small_sem.at[i]) for i, (src, dst) in enumerate(
        ((focus_in, focus), (onset_in, onset), (inv_in, inv), (fwd_in, fwd), (initial_in, initial)))]
    small[0].start()
    for h in range(CHUNKS):
        for name in PARTS:
            load(0, h, name).start()
            load(1, h, name).start()
        if h == 0:
            for copy in small[1:]:
                copy.start()

    barrier = pltpu.get_barrier_semaphore()
    for dz, dy in ((1, 0), (-1, 0), (0, 1), (0, -1)):
        pl.semaphore_signal(barrier, inc=1, device_id=(me_f, rec_of(dz, dy)), device_id_type=MESH)
    for d in range(1, NF):
        pl.semaphore_signal(barrier, inc=1, device_id=(lax.rem(me_f + d, NF), me_r), device_id_type=MESH)

    def onset_source(h):
        return lax.div(h * NZ * NY + me_r, CHUNKS)

    def onset_copy(u):
        index = me_r * CHUNKS + u
        target, h = lax.rem(index, NZ * NY), lax.div(index, NZ * NY)
        rows = onset.at[pl.ds(NR * u, NR), :]
        return target, h, rows, pltpu.make_async_remote_copy(
            src_ref=rows, dst_ref=onset_own.at[h], send_sem=onset_send.at[u], recv_sem=onset_recv.at[h],
            device_id=(me_f, target), device_id_type=MESH)

    for h in range(CHUNKS):
        @pl.when(onset_source(h) != me_r)
        def _():
            pl.semaphore_signal(barrier, inc=1, device_id=(me_f, onset_source(h)), device_id_type=MESH)

    def enter():
        for copy in small[1:]:
            copy.wait()
        peers = 4 + NF - 1
        for u in range(CHUNKS):
            peers += jnp.where(lax.rem(me_r * CHUNKS + u, NZ * NY) != me_r, 1, 0)
        pl.semaphore_wait(barrier, peers)
        for u in range(CHUNKS):
            target, h, rows, copy = onset_copy(u)

            @pl.when(target != me_r)
            def _():
                copy.start()

            @pl.when(target == me_r)
            def _():
                onset_own[h] = rows[...]

    def onset_ready():
        for u in range(CHUNKS):
            target, _h, _rows, copy = onset_copy(u)

            @pl.when(target != me_r)
            def _():
                copy.wait_send()

        for h in range(CHUNKS):
            @pl.when(onset_source(h) != me_r)
            def _():
                pltpu.make_async_remote_copy(
                    src_ref=onset_own.at[h], dst_ref=onset_own.at[h], send_sem=onset_send.at[0],
                    recv_sem=onset_recv.at[h], device_id=(me_f, me_r), device_id_type=MESH).wait_recv()

    lane = lax.broadcasted_iota(jnp.int32, (ROWS, 128), 1)
    low_half = lane < 64
    plan = Plan()
    copies = {}

    used, groups_of, units = {}, {}, {}

    def piece(name, src, dst, target, phase, h, size, group):
        bank = h if phase == 0 else (CHUNKS if h == 0 else h - 1)
        key = (phase, h, group or name)
        if key not in groups_of:
            used[phase, h] = used.get((phase, h), -1) + 1
            groups_of[key] = recv_sem.at[bank, used[phase, h]]
            units[key] = 0
        units[key] += size
        copies[name] = pltpu.make_async_remote_copy(
            src_ref=src, dst_ref=dst, send_sem=send_sem.at[phase], recv_sem=groups_of[key],
            device_id=(me_f, target), device_id_type=MESH)
        return copies[name]

    def wait_group(phase, h, group):
        key = (phase, h, group)
        amount = part.reshape(CHUNKS * FL * NZ * NY, NR, 128).at[pl.ds(0, units[key])]
        pltpu.make_async_copy(amount, amount, groups_of[key]).wait()

    def each(freqs, step, together):
        whole = len(freqs) // together * together if together else 0
        if whole > together:
            def body(i, carry):
                for k in range(together):
                    step(freqs[0] + i * together + k, 0)
                return carry

            lax.fori_loop(0, whole // together, body, 0)
        else:
            whole = 0
        for f in freqs[whole:]:
            step(f, 0)

    small[0].wait()
    for f in range(FL):
        value = focus[f]
        turned = pltpu.roll(value, 64, 1)
        xs[f, 0:ROWS, :] = value
        xs[f, ROWS : 2 * ROWS, :] = jnp.where(low_half, turned, -turned)

    def adjoint(freqs, h, name):
        def run():
            if freqs[0] == PARTS[name][0]:
                load(0, h, name).wait()
                load(1, h, name).wait()

            def step(f, _):
                x_high, x_low = split(xs[f])
                left = jnp.concatenate([x_high, x_high], axis=0)
                right = jnp.concatenate([x_low, jnp.zeros_like(x_low)], axis=0)
                both = jnp.concatenate([left, right], axis=1)
                for c in range(2):
                    high, low = split(resp[f, :, pl.ds(COLS * h + COLS // 2 * c, COLS // 2)])
                    terms = lax.dot_general(jnp.concatenate([high, low], axis=0), both, (((0,), (0,)), ((), ())),
                                            preferred_element_type=F32)
                    total = terms[:, :128] + terms[:, 128:]
                    part[f, h, NZ // 2 * c : NZ // 2 * (c + 1)] = total.reshape(NZ // 2, NY, NR, 128)
                return _

            each(freqs, step, ADJ)

        return run

    def groups(name, size):
        start, count = PARTS[name]
        return [tuple(range(f, min(f + size, start + count))) for f in range(start, start + count, size)]

    adjoint_done = {}
    for h in range(CHUNKS):
        for name in ("a", "b"):
            adjoint_done[h, name] = []
            for place, freqs in enumerate(groups(name, FL if h == 0 else 3)):
                key = f"adj{name}{h},{place}"
                adjoint_done[h, name].append(key)
                plan.add(key, (), adjoint(freqs, h, name), dur=3.4 / CHUNKS * len(freqs) / FL, rank=(0 if h == 0 else 1, max(h - 1, 0), 9, name != "a", place))

    slot = {"a1": 0, "a2": 0, "b1": 0, "b2": 0}
    stages = {"a1": stage_a1, "a2": stage_a2, "b1": stage_b1, "b2": stage_b2}

    def staging(kind, count):
        index = slot[kind]
        slot[kind] += 1
        return stages[kind].at[index, pl.ds(0, count)]

    def reduce_piece(name, kind, freqs, dz, dy, h, target, adds, deps, link, rank, group=None):
        start, count = freqs
        src = part.at[pl.ds(start, count), h, at_z(dz), at_y(dy)]
        dst = staging(kind, count)
        copy = piece(name, src, dst, target, 0, h, count, group)
        copies[name] = (copy, dst, start, count)

        def run():
            take(adds, dz, dy, h)
            copy.start()

        plan.add(name, tuple(adds) + tuple(deps), run, link, count * NR * 512, 0.12, rank)

    def take(adds, dz, dy, h, group=None):
        if group:
            wait_group(0, h, group)
        for other in adds:
            copy, dst, start, count = copies[other]
            if not group:
                copy.wait_recv()
            where = (pl.ds(start, count), h, at_z(dz), at_y(dy))
            part[where] += dst[...]

    for h in range(CHUNKS):
        deep = NZ // 2
        order_y = (2, 1, -1, 0)
        order_z = (4, 3, -3, 2, -2, 1, -1, 0)
        both_y = {1: (2, 0), -1: (1, -1)}
        both_z = {1: (4, 2, -2, 0), -1: (3, -3, 1, -1)}
        for k in range(deep, 0, -1):
            for place, dy in enumerate(order_y):
                for sign in (1, -1):
                    if k == deep and dy not in both_y[sign]:
                        continue
                    adds = [f"a1{h},{sign},{k + 1},{dy}"] if (k < deep - 1 or (k == deep - 1 and dy in both_y[sign])) else []
                    reduce_piece(f"a1{h},{sign},{k},{dy}", "a1", PARTS["a"], sign * k, dy, h, rec_of(sign, 0), adds,
                                 adjoint_done[h, "a"], ("z", sign), (1, h, 0, -k, place), f"a1{dy}" if k == 1 else None)
        for k in (2, 1):
            for place, dz in enumerate(order_z):
                for sign in (1, -1):
                    if k == 2 and dz not in both_z[sign]:
                        continue
                    adds = [f"b1{h},{sign},2,{dz}"] if k == 1 and dz in both_z[sign] else []
                    reduce_piece(f"b1{h},{sign},{k},{dz}", "b1", PARTS["b"], dz, sign * k, h, rec_of(0, sign), adds,
                                 adjoint_done[h, "b"], ("y", sign), (1, h, 0, -k, place), f"b1{dz}" if k == 1 else None)

        def first_sum(name, kind, d):
            keys = [f"{kind}{h},{sign},1,{d}" for sign in (1, -1)]

            def run(keys=keys, d=d, h=h, kind=kind):
                dz, dy = (0, d) if kind == "a1" else (d, 0)
                take(keys, dz, dy, h, f"{kind}{d}")

            plan.add(name, keys, run, dur=0.12, rank=(0, h, 0))

        for dy in order_y:
            first_sum(f"as{h},{dy}", "a1", dy)
        for dz in order_z:
            first_sum(f"bs{h},{dz}", "b1", dz)
        for sign in (1, -1):
            reduce_piece(f"a2{h},{sign},2", "a2", halves("a", sign), 0, 2 * sign, h, rec_of(0, sign), [],
                         (f"as{h},2",), ("y", sign), (0, h, 1, -2))
            reduce_piece(f"a2{h},{sign},1", "a2", PARTS["a"], 0, sign, h, rec_of(0, sign), [f"a2{h},{sign},2"],
                         (f"as{h},{sign}",), ("y", sign), (0, h, 1, -1), "own")
            for k in range(deep, 0, -1):
                freqs = halves("b", sign) if k == deep else PARTS["b"]
                adds = [] if k == deep else [f"b2{h},{sign},{k + 1}"]
                source = 4 if k == deep else sign * k
                reduce_piece(f"b2{h},{sign},{k}", "b2", freqs, sign * k, 0, h, rec_of(sign, 0), adds,
                             (f"bs{h},{source}",), ("z", sign), (0, h, 1, -k), "own" if k == 1 else None)

        own_keys = [f"a2{h},{sign},1" for sign in (1, -1)] + [f"b2{h},{sign},1" for sign in (1, -1)]

        def own_sum(keys=tuple(own_keys), h=h):
            take(keys, 0, 0, h, "own")

        plan.add(f"own{h}", own_keys + [f"as{h},0", f"bs{h},0"], own_sum, dur=0.2, rank=(0, h, 0))

    def block_of(buffer, h, j):
        return buffer.at[:, h, z, y, pl.ds(8 * (j - MEMBERS * h), 8), :]

    def out_copy(source, freqs, landing, row, j):
        start, count = freqs
        return pltpu.make_async_remote_copy(
            src_ref=source(j).at[pl.ds(start, count)], dst_ref=landing.at[pl.ds(FL * me_f + start, count)],
            send_sem=win_send.at[row], recv_sem=win_recv.at[row], device_id=(j, me_r), device_id_type=MESH)

    def return_copy(clipped, target, row, d):
        return pltpu.make_async_remote_copy(
            src_ref=clipped.at[pl.ds(FL * d, FL)], dst_ref=target(me_f),
            send_sem=ret_send.at[row], recv_sem=ret_recv.at[row], device_id=(d, me_r), device_id_type=MESH)

    def wait_tiles(buffer, count, sem):
        tiles = buffer.at[pl.ds(0, count)]
        pltpu.make_async_copy(tiles, tiles, sem).wait()

    def window(landing, clipped, starts):
        half = lax.broadcasted_iota(jnp.int32, (NF * FL, 128), 1) < 64
        tops, bottoms = [], []
        for m in range(4):
            first, second = landing[:, 2 * m, :], landing[:, 2 * m + 1, :]
            tops.append(jnp.where(half, first, pltpu.roll(second, 64, 1)))
            bottoms.append(jnp.where(half, pltpu.roll(first, 64, 1), second))
        spectrum = jnp.concatenate([jnp.concatenate(tops, axis=1), jnp.concatenate(bottoms, axis=1)], axis=0)
        high, low = split(spectrum)
        traces = jnp.dot(inv[...], jnp.concatenate([high, low, high], axis=0), preferred_element_type=F32)
        limit = starts()
        limits = jnp.concatenate([limit[m : m + 1, :] for m in range(8)], axis=1)
        sample = lax.broadcasted_iota(jnp.int32, traces.shape, 0)
        kept = jnp.where(sample < limits, traces, 0.0)
        high, low = split(kept)
        again = jnp.dot(fwd[...], jnp.concatenate([high, low, high], axis=0), preferred_element_type=F32)
        for m in range(4):
            real = again[: NF * FL, 128 * m : 128 * m + 128]
            imag = again[NF * FL :, 128 * m : 128 * m + 128]
            clipped[:, 2 * m, :] = jnp.where(half, real, pltpu.roll(imag, 64, 1))
            clipped[:, 2 * m + 1, :] = jnp.where(half, pltpu.roll(real, 64, 1), imag)

    def window_tasks(which, tag, members, source, sends, landing, clipped, starts, target, rank):
        inside = (me_f >= members[0]) & (me_f <= members[-1])
        returns = sends[0][1]

        def others(run):
            @pl.when(inside)
            def _():
                run(len(members) - 1)

            @pl.when(jnp.logical_not(inside))
            def _():
                run(len(members))

        def scatter(freqs, row):
            def run():
                for j in members:
                    @pl.when(me_f != j)
                    def _():
                        out_copy(source, freqs, landing, row, j).start()

                    @pl.when(me_f == j)
                    def _():
                        start, count = freqs
                        landing[FL * j + start : FL * j + start + count] = source(j)[start : start + count]

            return run

        def apply():
            @pl.when(inside)
            def _():
                for freqs, row, _deps in sends:
                    wait_tiles(landing, (NF - 1) * freqs[1], win_recv.at[row])
                window(landing, clipped, starts)
                for d in range(NF):
                    @pl.when(me_f != d)
                    def _():
                        return_copy(clipped, target, returns, d).start()

                target(me_f)[...] = clipped[pl.ds(FL * me_f, FL)]

        def drain():
            for freqs, row, _deps in sends:
                others(lambda n: wait_tiles(landing, n * freqs[1], win_send.at[row]))

            @pl.when(inside)
            def _():
                wait_tiles(landing, (NF - 1) * FL, ret_send.at[returns])

        def collect():
            others(lambda n: wait_tiles(landing, n * FL, ret_recv.at[returns]))
            if which == 1:
                drain()

        if which == 0:
            plan.add(tag + "drain", (tag + "in",) + ("w1in",), drain, dur=0.3, rank=(5,))
        outs = []
        for freqs, row, deps in sends:
            outs.append(f"{tag}out{row}")
            plan.add(outs[-1], deps, scatter(freqs, row), ("x", 0), len(members) * 8 * freqs[1] * 340, 0.2, rank if which == 0 else (2, 9))
        plan.add(tag + "win", outs, apply, ("x", 1), len(members) * 8 * FL * 340, 1.5, rank)
        plan.add(tag + "in", (tag + "win",), collect, dur=0.2, rank=rank)

    def onset_here():
        return onset[pl.ds(pl.multiple_of(8 * jnp.minimum(me_f, ROWS // 8 - 1), 8), 8), :]

    plan.add("onset", ("own0",), onset_ready, dur=0.05, rank=(0, 0, 0))
    for h in range(CHUNKS):
        def onset_summed(h=h):
            j = jnp.clip(me_f - MEMBERS * h, 0, MEMBERS - 1)
            return onset_own[h, pl.ds(pl.multiple_of(8 * j, 8), 8), :]

        members = tuple(range(MEMBERS * h, MEMBERS * h + MEMBERS))
        window_tasks(0, f"w{h}", members, functools.partial(block_of, part, h),
                     [((0, FL), h, (f"own{h}", "onset"))], x1, y1, onset_summed,
                     functools.partial(block_of, gathered, h), (0, h, 0))

    received, together = set(), set()

    def gather_piece(name, freqs, dz, dy, h, target, deps, link, rank, group=None):
        start, count = freqs
        where = gathered.at[pl.ds(start, count), h, at_z(dz), at_y(dy)]
        copy = piece(name, where, where, target, 1, h, count, group)
        if group:
            together.add(name)
        arrivals = [dep for dep in deps if dep in copies]

        def run():
            for dep in arrivals:
                receive(dep)
            copy.start()

        plan.add(name, deps, run, link, count * NR * 512, 0.08, rank)


    def receive(name):
        if name not in received and name not in together:
            received.add(name)
            copies[name].wait_recv()

    ends = {(h, name): [] for h in range(CHUNKS) for name in PARTS}
    for h in range(CHUNKS):
        own = f"w{h}in"
        deep = NZ // 2
        for sign in (1, -1):
            gather_piece(f"ya{h},{sign},0", PARTS["a"], 0, 0, h, rec_of(0, sign), (own,), ("y", sign), (2, 0, h))
            gather_piece(f"zb{h},{sign},0", PARTS["b"], 0, 0, h, rec_of(sign, 0), (own,), ("z", sign), (2, 0, h))
        for sign in (1, -1):
            gather_piece(f"ya{h},{sign},1", halves("a", sign), 0, -sign, h, rec_of(0, sign), (f"ya{h},{sign},0",),
                         ("y", sign), (2, 0, h))
            for k in range(1, deep):
                freqs = halves("b", sign) if k == deep - 1 else PARTS["b"]
                gather_piece(f"zb{h},{sign},{k}", freqs, -sign * k, 0, h, rec_of(sign, 0), (f"zb{h},{sign},{k - 1}",),
                             ("z", sign), (2, 0, h))
        for dy in (0, -1, 1, 2):
            if dy == 0:
                deps = (own,)
            elif dy == 2:
                deps = (f"ya{h},1,1", f"ya{h},-1,1")
            else:
                deps = (f"ya{h},{-dy},0",)
            for sign in (1, -1):
                for k in range(deep):
                    if k == deep - 1 and dy not in both_y[sign]:
                        continue
                    gather_piece(f"za{h},{sign},{k},{dy}", PARTS["a"], -sign * k, dy, h, rec_of(sign, 0),
                                 deps if k == 0 else (f"za{h},{sign},{k - 1},{dy}",), ("z", sign), (2, 1, h, k),
                                 None if k < deep - 2 or (k == deep - 2 and dy in both_y[sign]) else "a")
                    ends[h, "a"].append(f"za{h},{sign},{k},{dy}")
        for dz in (0, -1, 1, -2, 2, -3, 3, 4):
            if dz == 0:
                deps = (own,)
            elif dz == 4:
                deps = (f"zb{h},1,{deep - 1}", f"zb{h},-1,{deep - 1}")
            else:
                sign = -1 if dz > 0 else 1
                deps = (f"zb{h},{sign},{abs(dz) - 1}",)
            for sign in (1, -1):
                for k in range(2):
                    if k == 1 and dz not in both_z[sign]:
                        continue
                    gather_piece(f"yb{h},{sign},{k},{dz}", PARTS["b"], dz, -sign * k, h, rec_of(0, sign),
                                 deps if k == 0 else (f"yb{h},{sign},0,{dz}",), ("y", sign), (2, 1, h, k),
                                 None if k == 0 and dz in both_z[sign] else "b")
                    ends[h, "b"].append(f"yb{h},{sign},{k},{dz}")
        for name in list(copies):
            if name.startswith((f"ya{h}", f"zb{h}")):
                ends[h, name[1]].append(name)

    def forward(freqs, h, name):
        def run():
            if freqs[0] == PARTS[name][0]:
                for key in ends[h, name]:
                    receive(key)
                wait_group(1, h, name)

            def step(f, _):
                high, low = split(resp[f, :, pl.ds(COLS * h, COLS)])
                w_high, w_low = split(gathered[f, h].reshape(COLS, 128))
                terms = jnp.dot(jnp.concatenate([high, low], axis=0), jnp.concatenate([w_high, w_low], axis=1),
                                preferred_element_type=F32)
                total = terms[: 2 * ROWS, :128] + terms[: 2 * ROWS, 128:] + terms[2 * ROWS :, :128]
                if h > 0:
                    total = total + acc[f]
                if h < CHUNKS - 1:
                    acc[f] = total
                else:
                    turned = pltpu.roll(total[ROWS:], 64, 1)
                    made[f] = total[:ROWS] + jnp.where(low_half, -turned, turned)
                return _

            each(freqs, step, FWD)

        return run

    last = {}
    for h in range(CHUNKS):
        for name in PARTS:
            last[name] = []
            for place, freqs in enumerate(groups(name, 3 if h < CHUNKS - 1 else FL)):
                key = f"fwd{name}{h},{place}"
                last[name].append(key)
                before = [f"fwd{name}{h - 1},{p}" for p in range(len(groups(name, 3)))] if h else []
                plan.add(key, ends[h, name] + [f"w{h}in"] + before, forward(freqs, h, name),
                         dur=3.4 / CHUNKS * len(freqs) / FL, rank=(3, h))

    window_tasks(1, "v", tuple(range(ROWS // 8)), lambda j: made.at[:, pl.ds(8 * j, 8), :],
                 [(PARTS[name], CHUNKS + place, last[name]) for place, name in enumerate(("b", "a"))], x2, y2, onset_here,
                 lambda j: back.at[:, pl.ds(8 * j, 8), :], (4,))

    order = plan.order()
    entered = False
    for _now, name in order:
        if plan.tasks[name][2] and not entered:
            enter()
            entered = True
        plan.tasks[name][1]()
    blocks = CHUNKS * FL * (NZ * NY - 1)
    for phase, buffer in enumerate((part, gathered)):
        amount = buffer.reshape(CHUNKS * FL * NZ * NY, NR, 128).at[pl.ds(0, blocks)]
        pltpu.make_async_copy(amount, amount, send_sem.at[phase]).wait()
    out[...] = initial[...] - back[...]
    kernel.plan, kernel.used = plan, used
    kernel.ordered = order


def iterate(response_real, response_imaginary, focus, onset, inv, fwd, initial):
    na, nb = SPLIT, FL - SPLIT
    vmem = pl.BlockSpec(memory_space=pltpu.VMEM)
    scratch = [
        pltpu.VMEM(focus.shape, F32),
        pltpu.VMEM(onset.shape, jnp.int32),
        pltpu.VMEM(inv.shape, BF),
        pltpu.VMEM(fwd.shape, BF),
        pltpu.VMEM(focus.shape, F32),
        pltpu.SemaphoreType.DMA((5,)),
        pltpu.VMEM((FL, 2 * ROWS, response_real.shape[2]), F32),
        pltpu.SemaphoreType.DMA((2, CHUNKS, 2)),
        pltpu.VMEM((FL, CHUNKS, NZ, NY, NR, 128), F32),
        pltpu.VMEM((28 * CHUNKS, na, NR, 128), F32),
        pltpu.VMEM((4 * CHUNKS, na, NR, 128), F32),
        pltpu.VMEM((24 * CHUNKS, nb, NR, 128), F32),
        pltpu.VMEM((8 * CHUNKS, nb, NR, 128), F32),
        pltpu.VMEM((FL, CHUNKS, NZ, NY, NR, 128), F32),
        pltpu.VMEM((FL, 2 * ROWS, 128), F32),
        pltpu.VMEM((NF * FL, 8, 128), F32),
        pltpu.VMEM((NF * FL, 8, 128), F32),
        pltpu.VMEM((NF * FL, 8, 128), F32),
        pltpu.VMEM((NF * FL, 8, 128), F32),
        pltpu.VMEM((FL, 2 * ROWS, 128), F32),
        pltpu.VMEM((FL, ROWS, 128), F32),
        pltpu.VMEM((FL, ROWS, 128), F32),
        pltpu.VMEM((CHUNKS, NR, onset.shape[1]), jnp.int32),
        pltpu.SemaphoreType.DMA((CHUNKS,)),
        pltpu.SemaphoreType.DMA((CHUNKS,)),
        pltpu.SemaphoreType.DMA((2,)),
        pltpu.SemaphoreType.DMA((CHUNKS + 1, 49)),
        pltpu.SemaphoreType.DMA((CHUNKS + 2,)),
        pltpu.SemaphoreType.DMA((CHUNKS + 2,)),
        pltpu.SemaphoreType.DMA((CHUNKS + 1,)),
        pltpu.SemaphoreType.DMA((CHUNKS + 1,)),
    ]
    return pl.pallas_call(
        kernel,
        out_shape=jax.ShapeDtypeStruct((FL, ROWS, 128), F32),
        in_specs=[pl.BlockSpec(memory_space=pl.ANY)] * 7,
        out_specs=vmem,
        scratch_shapes=scratch,
        compiler_params=pltpu.CompilerParams(
            collective_id=0, has_side_effects=True, vmem_limit_bytes=60 * 1024 * 1024
        ),
    )(response_real, response_imaginary, focus, onset, inv, fwd, initial)


def on_device(response_real, response_imaginary, focus, initial, onset):
    inv, fwd = dft_tables(NF * FL)
    by_freq = jnp.transpose(focus, (1, 0, 2))
    update = iterate(response_real, response_imaginary, by_freq, onset, jnp.asarray(inv), jnp.asarray(fwd),
                     jnp.transpose(initial, (1, 0, 2)))
    return jnp.transpose(update, (1, 0, 2))


def solution(mesh):
    in_specs = (
        P("freq", "rec", None),
        P("freq", "rec", None),
        P("rec", "freq", None),
        P("rec", "freq", None),
        P("rec", None),
    )
    return jax.shard_map(
        on_device, mesh=mesh, in_specs=in_specs, out_specs=P("rec", "freq", None), check_vma=False
    )
```
